128 devices in a mesh: band: 32 (over z, y, x_hi), grid: 4 (over x_lo, core).
Axes of the slice: x: 4 (x_hi: 2, x_lo: 2; x = x_hi * 2 + x_lo), y: 4, z: 4, core: 2. Of those that a mesh axis runs over, the one named last changes fastest.
Arguments:
- orbitals: float32 [128, 110592], P('band', 'grid'), may hold values from -6 to 6
Outputs:
- exchange_vectors: float32 [128, 110592], P('band', 'grid')
- margin: float32 [128, 128], P('grid', 'band')
The draws below stay inside these ranges and needn't reach their ends.
All inputs are finite; a program needn't handle non-finite values.
Results may differ from the reference program's by a relative error of at most 0.00012.
Values sent between devices are 32-bit elements; how exact they have to be, the bound alone decides.
A program may use at most 128 MiB of HBM per device.

```python
import jax
import jax.numpy as jnp
from jax import lax

NG = 48
BAND_DEV = 4
NBANDS = 128
NCELL = 110592
N_BAND = 32


def steps_of(rng, dims, split, least, top_value):
    gain, own = 1.0, jax.random.fold_in(rng, 6)
    for position, shards_of in split:
        heights = jnp.exp(jax.random.uniform(jax.random.fold_in(own, position), (shards_of,), jnp.float32, least / len(split), top_value / len(split)))
        gain = gain * jnp.repeat(heights, dims[position] // shards_of).reshape([-1 if axis == position else 1 for axis in range(len(dims))])
    return gain


def normal_values(stream_key, shape, deviation, reach, split=(), kind=jnp.bfloat16):
    result = jax.random.normal(stream_key, shape, jnp.float32) * deviation
    if len(split) > 0:
        result = steps_of(stream_key, shape, split, -0.22, 0.18) * result
    return jnp.clip(result, min=-reach, max=reach).astype(kind)


def setup_inputs(seed: int = 0) -> dict:
    streams_of = jax.random.split(jax.random.key(seed), 2)
    orbitals = normal_values(streams_of[0], (NBANDS, NCELL), 1.0, 6.0, ((0, 32), (1, 4)), jnp.float32)
    return dict(orbitals=orbitals)


def folded_freq(count):
    indices = jnp.arange(count)
    return ((indices + count // 2) % count - count // 2).astype(jnp.float32)


def kernel_table():
    freqs = folded_freq(NG)
    squares = freqs[:, None, None] ** 2 + freqs[None, :, None] ** 2 + freqs[None, None, :] ** 2
    safe_sq = jnp.where(squares > 0, squares, jnp.float32(1.0))
    return jnp.where(squares > 0, 40.0 * (1.0 - jnp.exp(-squares / 16.0)) / safe_sq, jnp.float32(0.0))


def reference(orbitals):
    kernel = kernel_table()
    blocks = orbitals.reshape(N_BAND, BAND_DEV, NCELL)
    window = jnp.concatenate([blocks, jnp.roll(blocks, 1, axis=0), jnp.roll(blocks, -1, axis=0)], axis=1)

    def per_band(single, partners):
        density = (single[None, :] * partners).reshape(-1, NG, NG, NG)
        spectrum = jnp.fft.fftn(density, axes=(1, 2, 3))
        potential = jnp.real(jnp.fft.ifftn(spectrum * kernel, axes=(1, 2, 3))).reshape(-1, NCELL)
        return -jnp.sum(partners * potential, axis=0)

    def per_block(args):
        own_block, partners = args
        return lax.map(lambda single: per_band(single, partners), own_block)

    vectors = lax.map(per_block, (blocks, window)).reshape(NBANDS, NCELL).astype(jnp.float32)
    margin = jnp.dot(orbitals, vectors.T, precision=lax.Precision.HIGHEST, preferred_element_type=jnp.float32) / NCELL
    return vectors, margin
```

```python
import jax
import jax.numpy as jnp
import numpy as np
from jax import lax
from jax.experimental import pallas as pl
from jax.experimental.pallas import tpu as pltpu
from jax.sharding import PartitionSpec as P

NG = 48
NCELL = 110592
PITCH = 52
SLAB = 216
MESH = pl.DeviceIdType.MESH
F32 = jnp.float32
BF16 = jnp.bfloat16
U1, U2, U3, U5 = 3, 8, 8, 1
VMEM = pl.BlockSpec(memory_space=pltpu.VMEM)


def hartley_rows():
    index = np.arange(NG)
    angles = (index[:, None] * index[None, :] % NG) * (2 * np.pi / NG)
    table = (np.cos(angles) + np.sin(angles)).astype(np.float32)
    high = table.astype(BF16)
    low = (table - high.astype(np.float32)).astype(BF16)
    return jnp.asarray(np.concatenate([high, high, low], axis=1))


def folded(index):
    return ((index + NG // 2) % NG - NG // 2).astype(F32)


def kernel_rows():
    shape = (3, NG * NG, 128)
    tile, row, lane = (lax.broadcasted_iota(jnp.int32, shape, d) for d in range(3))
    x, y, z = folded((tile * 128 + lane) % NG), folded(row % NG), folded(row // NG)
    square = x * x + y * y + z * z
    safe = jnp.where(square > 0, square, 1.0)
    value = 40.0 * (1.0 - jnp.exp(-square / 16.0)) / safe / NCELL
    return jnp.where(square > 0, value, 0.0)


def place():
    b, g = lax.axis_index("band"), lax.axis_index("grid")
    return b, g


def at(b, g):
    return {"band": b, "grid": g}


def slab(g):
    return pl.ds(pl.multiple_of(g * SLAB, 8), SLAB)


def first_tile(m):
    return (27 * m) // 16


def chunk(m):
    return pl.ds(pl.multiple_of(8 * first_tile(m), 8), 16)


def meet(peers):
    barrier = pltpu.get_barrier_semaphore()
    for peer in peers:
        pl.semaphore_signal(barrier, inc=1, device_id=peer, device_id_type=MESH)
    return barrier


def gather_kernel(orb, a_out, b_out, o_out, below, send, recv, osend, orecv):
    b, g = place()
    m, xh, xl = b // 2, b % 2, g // 2
    across, core = at(b, (g + 2) % 4), at(b, g + 1 - 2 * (g % 2))
    up, down = at((b + 1) % 32, (g + 2) % 4), at((b + 31) % 32, (g + 2) % 4)
    far = (g + 2) % 4
    barrier = meet((across, core, up, down))

    def greet(k, _):
        peer = at(2 * ((m + k) % 16) + xh, g)
        pl.semaphore_signal(barrier, inc=1, device_id=peer, device_id_type=MESH)
        return 0

    lax.fori_loop(1, 16, greet, 0)
    pl.semaphore_wait(barrier, 19)

    def copy(src, dst, sem, peer):
        return pltpu.make_async_remote_copy(
            src_ref=src, dst_ref=dst, send_sem=send.at[sem], recv_sem=recv.at[sem],
            device_id=peer, device_id_type=MESH,
        )

    mine, theirs = slab(g), slab(far)
    a_across = copy(orb, a_out.at[:, mine, :], 0, across)
    b_up = copy(orb, below, 1, up)
    a_core = copy(orb, a_out.at[:, mine, :], 2, core)
    a_across.start()
    b_up.start()
    a_core.start()

    def other(k):
        n = (m + k) % 16
        return pltpu.make_async_remote_copy(
            src_ref=orb.at[:, chunk(n), :], dst_ref=o_out.at[m], send_sem=osend.at[k],
            recv_sem=orecv.at[k], device_id=at(2 * n + xh, g), device_id_type=MESH,
        )

    def scatter(k, _):
        other(k).start()
        return 0

    lax.fori_loop(1, 16, scatter, 0)
    a_out[:, mine, :] = orb[...]
    o_out[m] = orb[:, chunk(m), :]

    a_across.wait_recv()
    a_far = copy(a_out.at[:, theirs, :], a_out.at[:, theirs, :], 3, core)
    a_far.start()
    b_up.wait_recv()
    b_across = copy(below.at[pl.ds(2 - 2 * xl, 2)], b_out.at[:, theirs, :], 4, across)
    b_core = copy(below.at[pl.ds(2 * xl, 2)], b_out.at[:, theirs, :], 5, core)
    b_across.start()
    b_core.start()
    b_out[:, theirs, :] = below[pl.ds(2 * xl, 2)]
    b_across.wait_recv()
    b_far = copy(b_out.at[:, mine, :], b_out.at[:, mine, :], 6, core)
    b_far.start()
    for sent in (a_core, a_far, b_core, b_far):
        sent.wait_recv()
    for sent in (a_across, b_up, a_core, a_far, b_across, b_core, b_far):
        sent.wait_send()

    def gathered(k, _):
        other(k).wait()
        return 0

    lax.fori_loop(1, 16, gathered, 0)


def split(value):
    high = value.astype(BF16)
    low = (value - high.astype(F32)).astype(BF16)
    return high, low


def hartley(table, value):
    high, low = split(value)
    stack = jnp.concatenate([high, low, high], axis=0)
    dims = (((1,), (0,)), ((), ()))
    return lax.dot_general(table, stack, dims, preferred_element_type=F32)


def pair_kernel(a_ref, b_ref, h_ref, k_ref, va_ref, ob_ref, s_ref, r_ref):
    _, g = place()
    c, hx, d = g % 2, g // 2, 2 * (g % 2) + g // 2
    table = h_ref[...]

    def rows(t):
        return pl.ds(t, NG, stride=18)

    def load(ref, i, t):
        return jnp.concatenate([ref[i, rows(t), :], ref[i, rows(t + 1), :]], axis=1)

    def store(ref, j, t, value):
        ref[j, rows(t), :] = value[:, :128]
        ref[j, rows(t + 1), :] = value[:, 128:]

    def forward_x(i, _):
        for u in range(U1):
            t = (i * U1 + u) * 2
            a0, a1 = load(a_ref, 2 * c, t), load(a_ref, 2 * c + 1, t)
            b0, b1 = load(b_ref, 0, t), load(b_ref, 1, t)
            single = load(a_ref, d, t)
            for f in range(8):
                left = (a0, a0, a1, a1)[f] if f < 4 else single
                right = (b0, b1, b0, b1)[f] if f < 4 else load(a_ref, f - 4, t)
                out = hartley(table, left * right)
                s_ref[t, f * 48 : (f + 1) * 48, :] = out[:, :128]
                s_ref[t + 1, f * 48 : (f + 1) * 48, :] = out[:, 128:]
        return 0

    lax.fori_loop(0, 9 // U1, forward_x, 0)

    def turn_in(i, _):
        for v in range(3):
            for l in range(3):
                block = s_ref[i * 3 + v, l * 128 : (l + 1) * 128, :].T
                for n in range(16):
                    y, z = divmod(v * 128 + n * 8, 48)
                    r_ref[l, pl.ds((i * 8 + y) * PITCH + z, 8), :] = block[n * 8 : (n + 1) * 8, :]
        return 0

    lax.fori_loop(0, 6, turn_in, 0)

    def wide(ref, where):
        return jnp.concatenate([ref[0, where, :], ref[1, where, :], ref[2, where, :]], axis=1)

    def keep(where, value):
        for l in range(3):
            r_ref[l, where, :] = value[:, l * 128 : (l + 1) * 128]

    def along_z(i, _):
        for u in range(U2):
            where = pl.ds((i * U2 + u) * PITCH, 48)
            keep(where, hartley(table, wide(r_ref, where)))
        return 0

    def along_y(i, _):
        for u in range(U3):
            z = i * U3 + u
            where = pl.ds(z, 48, stride=PITCH)
            spectrum = hartley(table, wide(r_ref, where))
            keep(where, hartley(table, spectrum * wide(k_ref, pl.ds(z * 48, 48))))
        return 0

    lax.fori_loop(0, 48 // U2, along_z, 0)
    lax.fori_loop(0, 48 // U3, along_y, 0)
    lax.fori_loop(0, 48 // U2, along_z, 0)

    def turn_out(i, _):
        for v in range(3):
            for l in range(3):
                parts = []
                for n in range(16):
                    y, z = divmod(v * 128 + n * 8, 48)
                    parts.append(r_ref[l, pl.ds((i * 8 + y) * PITCH + z, 8), :])
                s_ref[i * 3 + v, l * 128 : (l + 1) * 128, :] = jnp.concatenate(parts, axis=0).T
        return 0

    lax.fori_loop(0, 6, turn_out, 0)

    def potential(f, t):
        span = slice(f * 48, (f + 1) * 48)
        return hartley(table, jnp.concatenate([s_ref[t, span, :], s_ref[t + 1, span, :]], axis=1))

    def backward_x(i, _):
        for u in range(U5):
            t = (i * U5 + u) * 2
            b0, b1 = load(b_ref, 0, t), load(b_ref, 1, t)
            p0, p1 = potential(0, t), potential(1, t)
            a0, a1 = load(a_ref, 2 * c, t), load(a_ref, 2 * c + 1, t)
            store(va_ref, 0, t, -(b0 * p0 + b1 * p1))
            p2, p3 = potential(2, t), potential(3, t)
            store(va_ref, 1, t, -(b0 * p2 + b1 * p3))
            store(ob_ref, 0, t, -(a0 * p0 + a1 * p2))
            store(ob_ref, 1, t, -(a0 * p1 + a1 * p3))
            total = load(va_ref, hx, t)
            for j in range(4):
                total = total - load(a_ref, j, t) * potential(4 + j, t)
            store(va_ref, hx, t, total)
        return 0

    lax.fori_loop(0, 9 // U5, backward_x, 0)


def reduce_kernel(va, ob, o_own, o_oth, v_out, m_out, owed1, sums, owed2, owed3, back1, sumv, back2,
                  vc, part, got, fin, turned, send, recv, vsend, vrecv, psend, precv, fsend, frecv):
    b, g = place()
    m, xh, xl, c = b // 2, b % 2, g // 2, g % 2
    far, near = (g + 2) % 4, g + 1 - 2 * c
    across, core = at(b, far), at(b, near)
    up, down = at((b + 1) % 32, far), at((b + 31) % 32, far)
    barrier = meet((across, core, up, down, at(b, 3 - g)))

    def greet(k, _):
        peer = at(2 * ((m + k) % 16) + xh, g)
        pl.semaphore_signal(barrier, inc=1, device_id=peer, device_id_type=MESH)
        return 0

    lax.fori_loop(1, 16, greet, 0)
    pl.semaphore_wait(barrier, 20)

    def copy(src, dst, sem, peer):
        return pltpu.make_async_remote_copy(
            src_ref=src, dst_ref=dst, send_sem=send.at[sem], recv_sem=recv.at[sem],
            device_id=peer, device_id_type=MESH,
        )

    other_half = pl.ds(pl.multiple_of((1 - xl) * 2 * SLAB, 8), 2 * SLAB)
    own_half = pl.multiple_of(xl * 2 * SLAB, 8)
    a0 = copy(va.at[0, other_half, :], back1.at[0], 0, across)
    a1 = copy(va.at[1, other_half, :], back1.at[1], 1, across)
    d0 = copy(ob.at[:, slab(1 - c), :], owed1.at[0], 2, core)
    d1 = copy(ob.at[:, slab(3 - c), :], owed1.at[1], 3, core)
    d0.start()
    d1.start()
    a0.start()
    d0.wait_recv()
    sums[0] = ob[:, slab(c), :] + owed1[0]
    d1.wait_recv()
    sums[1] = ob[:, slab(2 + c), :] + owed1[1]
    x2 = copy(sums.at[xl], owed2, 4, across)
    x2.start()
    y0 = copy(sums.at[1 - xl], owed3.at[xl], 5, down)
    y0.start()
    a1.start()
    x2.wait_recv()
    y1 = copy(owed2, owed3.at[1 - xl], 6, down)
    y1.start()
    a0.wait_recv()
    a1.wait_recv()
    for n in range(2):
        where = pl.ds(pl.multiple_of(own_half + n * SLAB, 8), SLAB)
        sumv[n] = va[:, where, :] + back1[:, n * SLAB : (n + 1) * SLAB, :]
    z0 = copy(sumv.at[1 - c], back2, 7, core)
    z0.start()
    y0.wait_recv()
    y1.wait_recv()
    v_out[pl.ds(2 * c, 2)] = sumv[c] + owed3[c]
    z0.wait_recv()
    v_out[pl.ds(2 - 2 * c, 2)] = back2[...] + owed3[1 - c]

    def other(k):
        n = (m + k) % 16
        return pltpu.make_async_remote_copy(
            src_ref=v_out.at[:, chunk(n), :], dst_ref=vc.at[m], send_sem=vsend.at[k],
            recv_sem=vrecv.at[k], device_id=at(2 * n + xh, g), device_id_type=MESH,
        )

    def scatter(k, _):
        other(k).start()
        return 0

    lax.fori_loop(1, 16, scatter, 0)
    vc[m] = v_out[:, chunk(m), :]
    for sent in (a0, a1, d0, d1, x2, y0, y1, z0):
        sent.wait_send()

    def gathered(k, _):
        other(k).wait()
        return 0

    lax.fori_loop(1, 16, gathered, 0)

    double = (first_tile(m + 1) - first_tile(m) - 1).astype(F32)
    dims = (((1,), (1,)), ((), ()))

    def products(r, total):
        own = jnp.concatenate([o_own[n, :, r, :] for n in range(16)], axis=0)
        oth = jnp.concatenate([o_oth[n, :, r, :] for n in range(16)], axis=0)
        vec = jnp.concatenate([vc[n, :, r, :] for n in range(16)], axis=0)
        vec = vec * jnp.where(r < 8, F32(1.0), double)
        both = jnp.concatenate([jnp.where(xh == 0, own, oth), jnp.where(xh == 0, oth, own)], axis=0)
        oh, ol = split(both)
        vh, vl = split(vec)
        left = jnp.concatenate([vh, vl, vh], axis=1)
        right = jnp.concatenate([oh, oh, ol], axis=1)
        return total + lax.dot_general(left, right, dims, preferred_element_type=F32)

    total = jnp.zeros((64, 128), F32)
    for r in range(16):
        total = products(r, total)
    part[...] = (total * (1.0 / NCELL)).reshape(8, 8, 128)

    def piece(k):
        n = (m + k) % 16
        return pltpu.make_async_remote_copy(
            src_ref=part.at[n // 2], dst_ref=got.at[k], send_sem=psend.at[k],
            recv_sem=precv.at[k], device_id=at(2 * n + xh, g), device_id_type=MESH,
        )

    def deal(k, _):
        piece(k).start()
        return 0

    lax.fori_loop(1, 16, deal, 0)

    def dealt(k, acc):
        piece(k).wait()
        return acc + got[k]

    fin[0] = lax.fori_loop(1, 16, dealt, part[m // 2])
    last = []
    for k in range(1, 4):
        peer = at(b, (g + k) % 4)
        last.append(pltpu.make_async_remote_copy(
            src_ref=fin.at[0], dst_ref=fin.at[k], send_sem=fsend.at[k], recv_sem=frecv.at[k],
            device_id=peer, device_id_type=MESH,
        ))
        last[-1].start()
    for sent in last:
        sent.wait()
    whole = fin[0] + fin[1] + fin[2] + fin[3]
    turned[...] = whole.T
    for mm in range(4):
        for half in range(2):
            rows = turned[pl.ds(half * 64 + 16 * g + 4 * mm, 4), :]
            m_out[8 * mm + 4 * half : 8 * mm + 4 * half + 4, :] = jnp.where(m % 2 == 0, rows[:, :4], rows[:, 4:])


def on_device(orbitals):
    shape = jax.ShapeDtypeStruct
    dma = pltpu.SemaphoreType.DMA
    planar = orbitals.reshape(4, SLAB, 128)
    whole_a, whole_b, o_own = pl.pallas_call(
        gather_kernel,
        out_shape=(shape((4, 864, 128), F32), shape((2, 864, 128), F32), shape((16, 4, 16, 128), F32)),
        in_specs=[VMEM],
        out_specs=(VMEM, VMEM, VMEM),
        scratch_shapes=[pltpu.VMEM((4, SLAB, 128), F32), dma((7,)), dma((7,)), dma((16,)), dma((16,))],
        compiler_params=pltpu.CompilerParams(collective_id=0, has_side_effects=True),
        name="gather",
    )(planar)
    pairs = [(n, n + 1 - 2 * (n % 2)) for n in range(32)]
    o_oth = lax.ppermute(o_own, "band", pairs)
    partial_a, partial_b = pl.pallas_call(
        pair_kernel,
        out_shape=(shape((2, 864, 128), F32), shape((2, 864, 128), F32)),
        in_specs=[VMEM] * 4,
        out_specs=(VMEM, VMEM),
        scratch_shapes=[pltpu.VMEM((18, 384, 128), F32), pltpu.VMEM((3, NG * PITCH, 128), F32)],
        compiler_params=pltpu.CompilerParams(vmem_limit_bytes=50 * 1024 * 1024),
        cost_estimate=pl.CostEstimate(flops=10**10, bytes_accessed=10**7, transcendentals=0),
        name="pairs",
    )(whole_a, whole_b, hartley_rows(), kernel_rows())
    half = pltpu.VMEM((2, 2, SLAB, 128), F32)
    vectors, margin = pl.pallas_call(
        reduce_kernel,
        out_shape=(shape((4, SLAB, 128), F32), shape((32, 4), F32)),
        in_specs=[VMEM] * 4,
        out_specs=(VMEM, VMEM),
        scratch_shapes=[
            half, half, pltpu.VMEM((2, SLAB, 128), F32), half, pltpu.VMEM((2, 2 * SLAB, 128), F32), half,
            pltpu.VMEM((2, SLAB, 128), F32), pltpu.VMEM((16, 4, 16, 128), F32), pltpu.VMEM((8, 8, 128), F32),
            pltpu.VMEM((16, 8, 128), F32), pltpu.VMEM((4, 8, 128), F32), pltpu.VMEM((128, 8), F32),
            dma((8,)), dma((8,)), dma((16,)), dma((16,)), dma((16,)), dma((16,)), dma((4,)), dma((4,)),
        ],
        compiler_params=pltpu.CompilerParams(collective_id=1, has_side_effects=True),
        name="reduce",
    )(partial_a, partial_b, o_own, o_oth)
    return vectors.reshape(4, SLAB * 128), margin


def solution(mesh):
    return jax.shard_map(
        on_device,
        mesh=mesh,
        in_specs=(P("band", "grid"),),
        out_specs=(P("band", "grid"), P("grid", "band")),
        check_vma=False,
    )
```

```python
import jax
import jax.numpy as jnp
import numpy as np
from jax import lax
from jax.experimental import pallas as pl
from jax.experimental.pallas import tpu as pltpu
from jax.sharding import PartitionSpec as P

NG = 48
NCELL = 110592
PITCH = 52
SLAB = 216
MESH = pl.DeviceIdType.MESH
F32 = jnp.float32
BF16 = jnp.bfloat16
U1, U2, U3, U5 = 3, 8, 8, 1
VMEM = pl.BlockSpec(memory_space=pltpu.VMEM)


def hartley_rows():
    index = np.arange(NG)
    angles = (index[:, None] * index[None, :] % NG) * (2 * np.pi / NG)
    table = (np.cos(angles) + np.sin(angles)).astype(np.float32)
    high = table.astype(BF16)
    low = (table - high.astype(np.float32)).astype(BF16)
    return jnp.asarray(np.concatenate([high, high, low], axis=1))


def folded(index):
    return ((index + NG // 2) % NG - NG // 2).astype(F32)


def at(b, g):
    return {"band": b, "grid": g}


def slab(g):
    return pl.ds(pl.multiple_of(g * SLAB, 8), SLAB)


def first_tile(m):
    return (27 * m) // 16


def split(value):
    high = value.astype(BF16)
    low = (value - high.astype(F32)).astype(BF16)
    return high, low


def hartley(table, value):
    high, low = split(value)
    stack = jnp.concatenate([high, low, high], axis=0)
    dims = (((1,), (0,)), ((), ()))
    return lax.dot_general(table, stack, dims, preferred_element_type=F32)


def fill_kernel(k_ref):
    lane = lax.broadcasted_iota(jnp.int32, (1, 128), 1)
    y = folded(lax.broadcasted_iota(jnp.int32, (NG, 128), 0))
    x = [folded((l * 128 + lane) % NG) for l in range(3)]
    planes = [y * y + v * v for v in x]

    def plane(z, _):
        depth = z.astype(F32)
        depth = depth * depth
        for l in range(3):
            square = planes[l] + depth
            safe = jnp.where(square > 0, square, 1.0)
            value = (40.0 / NCELL) * (1.0 - jnp.exp(-square / 16.0)) / safe
            value = jnp.where(square > 0, value, 0.0)
            k_ref[l, pl.ds(pl.multiple_of(z * NG, 8), NG), :] = value
        return 0

    lax.fori_loop(0, NG // 2 + 1, plane, 0)

    def mirror(z, _):
        for l in range(3):
            source = pl.ds(pl.multiple_of((NG - z) * NG, 8), NG)
            k_ref[l, pl.ds(pl.multiple_of(z * NG, 8), NG), :] = k_ref[l, source, :]
        return 0

    lax.fori_loop(NG // 2 + 1, NG, mirror, 0)


def exchange_kernel(orb, h_ref, v_out, m_out, a_ref, b_ref, below, o_own, o_oth, k_ref, s_ref, r_ref, va, ob,
                    owed1, sums, owed2, owed3, back1, sumv, back2, vec, vc, part, got, fin,
                    gsend, grecv, osend, orecv, send, recv, vsend, vrecv, psend, precv, fsend, frecv):
    b, g = lax.axis_index("band"), lax.axis_index("grid")
    m, xh, xl, c = b // 2, b % 2, g // 2, g % 2
    far, near = (g + 2) % 4, g + 1 - 2 * c
    across, core = at(b, far), at(b, near)
    up, down = at((b + 1) % 32, far), at((b + 31) % 32, far)
    twin = at(b + 1 - 2 * xh, g)
    mine, theirs = slab(g), slab(far)
    barrier = pltpu.get_barrier_semaphore()
    for peer in (across, core, up, down, at(b, 3 - g), twin):
        pl.semaphore_signal(barrier, inc=1, device_id=peer, device_id_type=MESH)

    def greet(k, _):
        peer = at(2 * ((m + k) % 16) + xh, g)
        pl.semaphore_signal(barrier, inc=1, device_id=peer, device_id_type=MESH)
        return 0

    lax.fori_loop(1, 16, greet, 0)
    for n in range(4):
        a_ref[n, mine, :] = orb[pl.ds(n, SLAB, stride=4), :]
    pl.semaphore_wait(barrier, 21)

    def remote(sends, recvs, sem, src, dst, peer):
        return pltpu.make_async_remote_copy(
            src_ref=src, dst_ref=dst, send_sem=sends.at[sem], recv_sem=recvs.at[sem],
            device_id=peer, device_id_type=MESH,
        )

    def first(sem, src, dst, peer):
        return remote(gsend, grecv, sem, src, dst, peer)

    def copy(sem, src, dst, peer):
        return remote(send, recv, sem, src, dst, peer)

    def own_a(n):
        return a_ref.at[pl.ds(2 * n, 2), mine, :]

    def far_a(n):
        return a_ref.at[pl.ds(2 * n, 2), theirs, :]

    with jax.named_scope("gather_a"):
        a_across = [first(n, own_a(n), own_a(n), across) for n in range(2)]
        a_core = first(2, a_ref.at[:, mine, :], a_ref.at[:, mine, :], core)
        a_far = [first(3 + n, far_a(n), far_a(n), core) for n in range(2)]
        b_up = first(5, a_ref.at[:, mine, :], below, up)
        b_across = first(6, below.at[pl.ds(2 - 2 * xl, 2)], b_ref.at[:, theirs, :], across)
        b_core = first(7, below.at[pl.ds(2 * xl, 2)], b_ref.at[:, theirs, :], core)
        b_far = first(8, b_ref.at[:, mine, :], b_ref.at[:, mine, :], core)
        for started in (a_across[0], a_across[1], b_up, a_core):
            started.start()

        def chunk(n):
            return pl.ds(pl.multiple_of(g * SLAB + 8 * first_tile(n), 8), 16)

        o_own[m] = a_ref[:, chunk(m), :]
        fill_kernel(k_ref)
        for n in range(2):
            a_across[n].wait_recv()
            a_far[n].start()
        b_up.wait_recv()
        b_across.start()
        b_core.start()

        def other(k):
            n = (m + k) % 16
            return remote(osend, orecv, k, a_ref.at[:, chunk(n), :], o_own.at[m], at(2 * n + xh, g))

        def scatter(k, _):
            other(k).start()
            return 0

        lax.fori_loop(1, 16, scatter, 0)
        b_ref[:, theirs, :] = below[pl.ds(2 * xl, 2)]
        a_core.wait_recv()
        a_far[0].wait_recv()
        a_far[1].wait_recv()

    d = 2 * c + xl
    table = h_ref[...]

    def rows(t):
        return pl.ds(t, NG, stride=18)

    def load(ref, i, t):
        return jnp.concatenate([ref[i, rows(t), :], ref[i, rows(t + 1), :]], axis=1)

    def store(ref, j, t, value):
        ref[j, rows(t), :] = value[:, :128]
        ref[j, rows(t + 1), :] = value[:, 128:]

    def forward(f, t, product):
        out = hartley(table, product)
        s_ref[t, f * 48 : (f + 1) * 48, :] = out[:, :128]
        s_ref[t + 1, f * 48 : (f + 1) * 48, :] = out[:, 128:]

    def forward_own(i, _):
        for u in range(U1):
            t = (i * U1 + u) * 2
            single = load(a_ref, d, t)
            for f in range(4):
                forward(4 + f, t, single * load(a_ref, f, t))
        return 0

    def forward_below(i, _):
        for u in range(U1):
            t = (i * U1 + u) * 2
            a0, a1 = load(a_ref, 2 * c, t), load(a_ref, 2 * c + 1, t)
            b0, b1 = load(b_ref, 0, t), load(b_ref, 1, t)
            for f, product in enumerate((a0 * b0, a0 * b1, a1 * b0, a1 * b1)):
                forward(f, t, product)
        return 0

    with jax.named_scope("forward_own"):
        lax.fori_loop(0, 9 // U1, forward_own, 0)
    with jax.named_scope("wait_b"):
        b_across.wait_recv()
        b_far.start()
        b_core.wait_recv()
        b_far.wait_recv()
    with jax.named_scope("forward_below"):
        lax.fori_loop(0, 9 // U1, forward_below, 0)

    def turn_in(i, _):
        for v in range(3):
            for l in range(3):
                block = s_ref[i * 3 + v, l * 128 : (l + 1) * 128, :].T
                for n in range(16):
                    y, z = divmod(v * 128 + n * 8, 48)
                    r_ref[l, pl.ds((i * 8 + y) * PITCH + z, 8), :] = block[n * 8 : (n + 1) * 8, :]
        return 0

    with jax.named_scope("turn_in"):
        lax.fori_loop(0, 6, turn_in, 0)

    def wide(ref, where):
        return jnp.concatenate([ref[0, where, :], ref[1, where, :], ref[2, where, :]], axis=1)

    def keep(where, value):
        for l in range(3):
            r_ref[l, where, :] = value[:, l * 128 : (l + 1) * 128]

    def along_z(i, _):
        for u in range(U2):
            where = pl.ds((i * U2 + u) * PITCH, 48)
            keep(where, hartley(table, wide(r_ref, where)))
        return 0

    def along_y(i, _):
        for u in range(U3):
            z = i * U3 + u
            where = pl.ds(z, 48, stride=PITCH)
            spectrum = hartley(table, wide(r_ref, where))
            keep(where, hartley(table, spectrum * wide(k_ref, pl.ds(z * 48, 48))))
        return 0

    with jax.named_scope("along_z"):
        lax.fori_loop(0, 48 // U2, along_z, 0)
    with jax.named_scope("along_y"):
        lax.fori_loop(0, 48 // U3, along_y, 0)

    with jax.named_scope("o_wait"):

        def gathered(k, _):
            other(k).wait()
            return 0

        lax.fori_loop(1, 16, gathered, 0)
        o_twin = first(9, o_own, o_oth, twin)
        o_twin.start()

    with jax.named_scope("along_z"):
        lax.fori_loop(0, 48 // U2, along_z, 0)

    def turn_out(i, _):
        for v in range(3):
            for l in range(3):
                parts = []
                for n in range(16):
                    y, z = divmod(v * 128 + n * 8, 48)
                    parts.append(r_ref[l, pl.ds((i * 8 + y) * PITCH + z, 8), :])
                s_ref[i * 3 + v, l * 128 : (l + 1) * 128, :] = jnp.concatenate(parts, axis=0).T
        return 0

    with jax.named_scope("turn_out"):
        lax.fori_loop(0, 6, turn_out, 0)

    def potential(f, t):
        span = slice(f * 48, (f + 1) * 48)
        return hartley(table, jnp.concatenate([s_ref[t, span, :], s_ref[t + 1, span, :]], axis=1))

    def backward_x(i, _):
        for u in range(U5):
            t = (i * U5 + u) * 2
            b0, b1 = load(b_ref, 0, t), load(b_ref, 1, t)
            p0, p1 = potential(0, t), potential(1, t)
            a0, a1 = load(a_ref, 2 * c, t), load(a_ref, 2 * c + 1, t)
            store(va, 0, t, -(b0 * p0 + b1 * p1))
            p2, p3 = potential(2, t), potential(3, t)
            store(va, 1, t, -(b0 * p2 + b1 * p3))
            store(ob, 0, t, -(a0 * p0 + a1 * p2))
            store(ob, 1, t, -(a0 * p1 + a1 * p3))
            total = load(va, xl, t)
            for j in range(4):
                total = total - load(a_ref, j, t) * potential(4 + j, t)
            store(va, xl, t, total)
        return 0

    with jax.named_scope("backward_x"):
        lax.fori_loop(0, 9 // U5, backward_x, 0)

    with jax.named_scope("reduce_owed"):
        other_half = pl.ds(pl.multiple_of((1 - xl) * 2 * SLAB, 8), 2 * SLAB)
        own_half = pl.multiple_of(xl * 2 * SLAB, 8)
        a0 = copy(0, va.at[0, other_half, :], back1.at[0], across)
        a1 = copy(1, va.at[1, other_half, :], back1.at[1], across)
        d0 = copy(2, ob.at[:, slab(1 - c), :], owed1.at[0], core)
        d1 = copy(3, ob.at[:, slab(3 - c), :], owed1.at[1], core)
        d0.start()
        d1.start()
        a0.start()
        d0.wait_recv()
        sums[0] = ob[:, slab(c), :] + owed1[0]
        d1.wait_recv()
        sums[1] = ob[:, slab(2 + c), :] + owed1[1]
        x2 = copy(4, sums.at[xl], owed2, across)
        x2.start()
        y0 = copy(5, sums.at[1 - xl], owed3.at[xl], down)
        y0.start()
        a1.start()
        x2.wait_recv()
        y1 = copy(6, owed2, owed3.at[1 - xl], down)
        y1.start()
    with jax.named_scope("reduce_a"):
        a0.wait_recv()
        a1.wait_recv()
        for n in range(2):
            where = pl.ds(pl.multiple_of(own_half + n * SLAB, 8), SLAB)
            sumv[n] = va[:, where, :] + back1[:, n * SLAB : (n + 1) * SLAB, :]
        z0 = copy(7, sumv.at[1 - c], back2, core)
        z0.start()
    with jax.named_scope("reduce_last"):
        y0.wait_recv()
        y1.wait_recv()
        vec[pl.ds(2 * c, 2)] = sumv[c] + owed3[c]
        z0.wait_recv()
        vec[pl.ds(2 - 2 * c, 2)] = back2[...] + owed3[1 - c]

    def piece_of(n):
        return pl.ds(pl.multiple_of(8 * first_tile(n), 8), 16)

    def spread(k):
        n = (m + k) % 16
        return remote(vsend, vrecv, k, vec.at[:, piece_of(n), :], vc.at[m], at(2 * n + xh, g))

    def spread_start(k, _):
        spread(k).start()
        return 0

    with jax.named_scope("spread_v"):
        lax.fori_loop(1, 16, spread_start, 0)
        vc[m] = vec[:, piece_of(m), :]
        for n in range(4):
            v_out[pl.ds(n, SLAB, stride=4), :] = vec[n]
        for sent in (*a_across, a_core, *a_far, b_up, b_across, b_core, b_far, a0, a1, d0, d1, x2, y0, y1, z0):
            sent.wait_send()
        o_twin.wait()

        def spread_wait(k, _):
            spread(k).wait()
            return 0

        lax.fori_loop(1, 16, spread_wait, 0)

    double = (first_tile(m + 1) - first_tile(m) - 1).astype(F32)
    dims = (((1,), (1,)), ((), ()))

    def products(r, total):
        both = []
        for n in range(16):
            own, oth = o_own[n, :, r, :], o_oth[n, :, r, :]
            both += [jnp.where(xh == 0, own, oth), jnp.where(xh == 0, oth, own)]
        some = jnp.concatenate([vc[n, :, r, :] for n in range(16)], axis=0)
        if r >= 8:
            some = some * double
        oh, ol = split(jnp.concatenate(both, axis=0))
        vh, vl = split(some)
        left = jnp.concatenate([vh, vl, vh], axis=1)
        right = jnp.concatenate([oh, oh, ol], axis=1)
        return total + lax.dot_general(left, right, dims, preferred_element_type=F32)

    with jax.named_scope("products"):
        total = jnp.zeros((64, 128), F32)
        for r in range(16):
            total = products(r, total)
        part[...] = (total * (1.0 / NCELL)).reshape(8, 8, 128)

    def piece(k):
        n = (m + k) % 16
        return remote(psend, precv, k, part.at[n // 2], got.at[k], at(2 * n + xh, g))

    def deal(k, _):
        piece(k).start()
        return 0

    def dealt(k, acc):
        piece(k).wait()
        return acc + got[k]

    with jax.named_scope("deal"):
        lax.fori_loop(1, 16, deal, 0)
        fin[0] = lax.fori_loop(1, 16, dealt, part[m // 2])
    with jax.named_scope("last"):
        last = [remote(fsend, frecv, k, fin.at[0], fin.at[k], at(b, (g + k) % 4)) for k in range(1, 4)]
        for sent in last:
            sent.start()
        for sent in last:
            sent.wait()
        whole = fin[0] + fin[1] + fin[2] + fin[3]
        quarter = jnp.where(m % 2 == 0, whole[:4], whole[4:])
        low = jnp.where(g % 2 == 0, quarter[:, :32], quarter[:, 32:64])
        high = jnp.where(g % 2 == 0, quarter[:, 64:96], quarter[:, 96:])
        m_out[...] = jnp.where(g < 2, low, high)


def on_device(orbitals):
    shape = jax.ShapeDtypeStruct
    dma = pltpu.SemaphoreType.DMA

    def room(*dims):
        return pltpu.VMEM(dims, F32)

    packed = orbitals.reshape(4, SLAB, 128).transpose(1, 0, 2).reshape(4 * SLAB, 128)
    half = room(2, 2, SLAB, 128)
    vectors, margin = pl.pallas_call(
        exchange_kernel,
        out_shape=(shape((4 * SLAB, 128), F32), shape((4, 32), F32)),
        in_specs=[VMEM] * 2,
        out_specs=(VMEM, VMEM),
        scratch_shapes=[
            room(4, 864, 128), room(2, 864, 128), room(4, SLAB, 128),
            room(16, 4, 16, 128), room(16, 4, 16, 128), room(3, NG * NG, 128),
            room(18, 384, 128), room(3, NG * PITCH, 128), room(2, 864, 128), room(2, 864, 128),
            half, half, room(2, SLAB, 128), half, room(2, 2 * SLAB, 128), half,
            room(2, SLAB, 128), room(4, SLAB, 128), room(16, 4, 16, 128), room(8, 8, 128),
            room(16, 8, 128), room(4, 8, 128),
            dma((10,)), dma((10,)), dma((16,)), dma((16,)), dma((8,)), dma((8,)),
            dma((16,)), dma((16,)), dma((16,)), dma((16,)), dma((4,)), dma((4,)),
        ],
        compiler_params=pltpu.CompilerParams(
            collective_id=0, has_side_effects=True, vmem_limit_bytes=50 * 1024 * 1024
        ),
        name="exchange",
    )(packed, hartley_rows())
    vectors = vectors.reshape(SLAB, 4, 128).transpose(1, 0, 2).reshape(4, SLAB * 128)
    return vectors, margin.T


def solution(mesh):
    return jax.shard_map(
        on_device,
        mesh=mesh,
        in_specs=(P("band", "grid"),),
        out_specs=(P("band", "grid"), P("grid", "band")),
        check_vma=False,
    )
```

```python
import jax
import jax.numpy as jnp
import numpy as np
from jax import lax
from jax.experimental import pallas as pl
from jax.experimental.pallas import tpu as pltpu
from jax.sharding import PartitionSpec as P

NG = 48
NCELL = 110592
PITCH = 52
SLAB = 216
MESH = pl.DeviceIdType.MESH
F32 = jnp.float32
BF16 = jnp.bfloat16
U1, U2, U3, U5 = 3, 8, 8, 1
VMEM = pl.BlockSpec(memory_space=pltpu.VMEM)


def hartley_rows():
    index = np.arange(NG)
    angles = (index[:, None] * index[None, :] % NG) * (2 * np.pi / NG)
    table = (np.cos(angles) + np.sin(angles)).astype(np.float32)
    high = table.astype(BF16)
    low = (table - high.astype(np.float32)).astype(BF16)
    return jnp.asarray(np.concatenate([high, high, low], axis=1))


def folded(index):
    return ((index + NG // 2) % NG - NG // 2).astype(F32)


def at(b, g):
    return {"band": b, "grid": g}


def slab(g):
    return pl.ds(pl.multiple_of(g * SLAB, 8), SLAB)


def first_tile(m):
    return (27 * m) // 16


def split(value):
    high = value.astype(BF16)
    low = (value - high.astype(F32)).astype(BF16)
    return high, low


def hartley(table, value):
    high, low = split(value)
    stack = jnp.concatenate([high, low, high], axis=0)
    dims = (((1,), (0,)), ((), ()))
    return lax.dot_general(table, stack, dims, preferred_element_type=F32)


def fill_kernel(k_ref):
    lane = lax.broadcasted_iota(jnp.int32, (1, 128), 1)
    y = folded(lax.broadcasted_iota(jnp.int32, (NG, 128), 0))
    x = [folded((l * 128 + lane) % NG) for l in range(3)]
    planes = [y * y + v * v for v in x]

    def plane(z, _):
        depth = z.astype(F32)
        depth = depth * depth
        for l in range(3):
            square = planes[l] + depth
            safe = jnp.where(square > 0, square, 1.0)
            value = (40.0 / NCELL) * (1.0 - jnp.exp(-square / 16.0)) / safe
            value = jnp.where(square > 0, value, 0.0)
            k_ref[l, pl.ds(pl.multiple_of(z * NG, 8), NG), :] = value
        return 0

    lax.fori_loop(0, NG // 2 + 1, plane, 0)

    def mirror(z, _):
        for l in range(3):
            source = pl.ds(pl.multiple_of((NG - z) * NG, 8), NG)
            k_ref[l, pl.ds(pl.multiple_of(z * NG, 8), NG), :] = k_ref[l, source, :]
        return 0

    lax.fori_loop(NG // 2 + 1, NG, mirror, 0)


def exchange_kernel(orb_hbm, h_hbm, v_out, m_out, orb, h_ref, load_sem, a_ref, b_ref, o_all, k_ref, s_ref, r_ref, q_ref,
                    va, ob, owed1, sums, owed3, back1, back2, back3, vec, vc, part, near_part, rows_out, rows_in,
                    gsend, grecv, osend, orecv, send, recv, vsend, vrecv, psend, precv, nsend, nrecv):
    b, g = lax.axis_index("band"), lax.axis_index("grid")
    m, xh, xl, c = b // 2, b % 2, g // 2, g % 2
    far, near = (g + 2) % 4, g + 1 - 2 * c
    across, core, diagonal = at(b, far), at(b, near), at(b, 3 - g)
    up, up_far = at((b + 1) % 32, g), at((b + 1) % 32, far)
    down, down_far = at((b + 31) % 32, g), at((b + 31) % 32, far)
    twin = at(b + 1 - 2 * xh, g)
    mine, theirs = slab(g), slab(far)
    fetch = pltpu.make_async_copy(orb_hbm, orb, load_sem.at[0])
    fetch.start()
    fetch_table = pltpu.make_async_copy(h_hbm, h_ref, load_sem.at[1])
    fetch_table.start()
    barrier = pltpu.get_barrier_semaphore()
    for peer in (up, up_far, down, down_far):
        pl.semaphore_signal(barrier, inc=1, device_id=peer, device_id_type=MESH)

    for peer in (across, core, diagonal):
        pl.semaphore_signal(barrier, inc=1, device_id=peer, device_id_type=MESH)

    def greet(k, _):
        peer = at(2 * ((m + k) % 16) + xh, g)
        pl.semaphore_signal(barrier, inc=1, device_id=peer, device_id_type=MESH)
        return 0

    lax.fori_loop(1, 16, greet, 0)
    fetch.wait()
    for n in range(4):
        a_ref[n, mine, :] = orb[pl.ds(n, SLAB, stride=4), :]
    pl.semaphore_wait(barrier, 22)

    def remote(sends, recvs, sem, src, dst, peer, recv_at=None):
        return pltpu.make_async_remote_copy(
            src_ref=src, dst_ref=dst, send_sem=sends.at[sem], recv_sem=recvs.at[sem if recv_at is None else recv_at],
            device_id=peer, device_id_type=MESH,
        )

    def first(sem, src, dst, peer):
        return remote(gsend, grecv, sem, src, dst, peer)

    def copy(sem, src, dst, peer):
        return remote(send, recv, sem, src, dst, peer)

    def own_a(n):
        return a_ref.at[pl.ds(2 * n, 2), mine, :]

    def far_a(n):
        return a_ref.at[pl.ds(2 * n, 2), theirs, :]

    with jax.named_scope("gather_a"):
        a_across = [first(n, own_a(n), own_a(n), across) for n in range(2)]
        a_core = first(2, a_ref.at[:, mine, :], a_ref.at[:, mine, :], core)
        a_far = [first(3 + n, far_a(n), far_a(n), core) for n in range(2)]
        b_near = first(5, a_ref.at[pl.ds(2 - 2 * xl, 2), mine, :], b_ref.at[:, mine, :], up_far)
        b_wide = first(6, a_ref.at[pl.ds(2 * xl, 2), mine, :], b_ref.at[:, mine, :], up)
        b_core = first(7, b_ref.at[:, theirs, :], b_ref.at[:, theirs, :], core)
        b_far = first(8, b_ref.at[:, mine, :], b_ref.at[:, mine, :], core)
        for started in (a_across[0], b_wide, a_across[1], b_near, a_core):
            started.start()

        def chunk(n):
            return pl.ds(pl.multiple_of(g * SLAB + 8 * first_tile(n), 8), 16)

        def other(k):
            n = (m + k) % 16
            return remote(osend, orecv, k, a_ref.at[:, chunk(n), :], o_all.at[m, xh], at(2 * n + xh, g))

        def scatter(k, _):
            other(k).start()
            return 0

        lax.fori_loop(1, 16, scatter, 0)
        o_all[m, xh] = a_ref[:, chunk(m), :]
        fill_kernel(k_ref)
        a_across[0].wait_recv()
        a_far[0].start()
        b_near.wait_recv()
        b_core.start()
        a_across[1].wait_recv()
        a_far[1].start()
        a_core.wait_recv()
        a_far[0].wait_recv()
        a_far[1].wait_recv()

    d = 2 * c + xl
    fetch_table.wait()
    table = h_ref[...]

    def rows(t):
        return pl.ds(t, NG, stride=18)

    def load(ref, i, t):
        return jnp.concatenate([ref[i, rows(t), :], ref[i, rows(t + 1), :]], axis=1)

    def store(ref, j, t, value):
        ref[j, rows(t), :] = value[:, :128]
        ref[j, rows(t + 1), :] = value[:, 128:]

    def forward(f, t, product):
        out = hartley(table, product)
        s_ref[t, f * 48 : (f + 1) * 48, :] = out[:, :128]
        s_ref[t + 1, f * 48 : (f + 1) * 48, :] = out[:, 128:]

    def forward_own(i, _):
        for u in range(U1):
            t = (i * U1 + u) * 2
            single = load(a_ref, d, t)
            for f in range(4):
                forward(4 + f, t, single * load(a_ref, f, t))
        return 0

    def forward_below(i, _):
        for u in range(U1):
            t = (i * U1 + u) * 2
            a0, a1 = load(a_ref, 2 * c, t), load(a_ref, 2 * c + 1, t)
            b0, b1 = load(b_ref, 0, t), load(b_ref, 1, t)
            for f, product in enumerate((a0 * b0, a0 * b1, a1 * b0, a1 * b1)):
                forward(f, t, product)
        return 0

    with jax.named_scope("forward_own"):
        lax.fori_loop(0, 9 // U1, forward_own, 0)
    with jax.named_scope("wait_b"):
        b_wide.wait_recv()
        b_far.start()

        b_core.wait_recv()
        b_far.wait_recv()
    with jax.named_scope("o_wait"):

        def gathered(k, _):
            other(k).wait()
            return 0

        lax.fori_loop(1, 16, gathered, 0)
        o_twin = first(9, o_all.at[:, xh], o_all.at[:, xh], twin)
        o_twin.start()

    with jax.named_scope("forward_below"):
        lax.fori_loop(0, 9 // U1, forward_below, 0)

    def turn_in(i, _):
        for v in range(3):
            for l in range(3):
                block = s_ref[i * 3 + v, l * 128 : (l + 1) * 128, :].T
                for n in range(16):
                    y, z = divmod(v * 128 + n * 8, 48)
                    r_ref[l, pl.ds((i * 8 + y) * PITCH + z, 8), :] = block[n * 8 : (n + 1) * 8, :]
        return 0

    with jax.named_scope("turn_in"):
        lax.fori_loop(0, 6, turn_in, 0)

    def passes(source, target, where, count, scale=None):
        tiles = [(u, l) for u in range(count) for l in range(3)]
        for p in range(0, len(tiles), 2):
            pair = tiles[p : p + 2]
            value = jnp.concatenate([source[l, where(u), :] for u, l in pair], axis=1)
            out = hartley(table, value)
            for j, (u, l) in enumerate(pair):
                piece = out[:, 128 * j : 128 * (j + 1)]
                if scale is not None:
                    piece = piece * k_ref[l, scale(u), :]
                target[l, where(u), :] = piece

    def along_z(source, target):
        def step(i, _):
            passes(source, target, lambda u: pl.ds((i * U2 + u) * PITCH, 48), U2)
            return 0

        lax.fori_loop(0, 48 // U2, step, 0)

    def along_y(source, target, scaled):
        def step(i, _):
            passes(source, target, lambda u: pl.ds(i * U3 + u, 48, stride=PITCH), U3,
                   (lambda u: pl.ds(pl.multiple_of((i * U3 + u) * 48, 8), 48)) if scaled else None)
            return 0

        lax.fori_loop(0, 48 // U3, step, 0)

    with jax.named_scope("along_z"):
        along_z(r_ref, q_ref)
    with jax.named_scope("along_y"):
        along_y(q_ref, r_ref, True)
    with jax.named_scope("along_y"):
        along_y(r_ref, q_ref, False)
    with jax.named_scope("along_z"):
        along_z(q_ref, r_ref)

    def turn_out(i, _):
        for v in range(3):
            for l in range(3):
                parts = []
                for n in range(16):
                    y, z = divmod(v * 128 + n * 8, 48)
                    parts.append(r_ref[l, pl.ds((i * 8 + y) * PITCH + z, 8), :])
                s_ref[i * 3 + v, l * 128 : (l + 1) * 128, :] = jnp.concatenate(parts, axis=0).T
        return 0

    with jax.named_scope("turn_out"):
        lax.fori_loop(0, 6, turn_out, 0)

    def potential(f, t):
        span = slice(f * 48, (f + 1) * 48)
        return hartley(table, jnp.concatenate([s_ref[t, span, :], s_ref[t + 1, span, :]], axis=1))

    def backward_below(i, _):
        for u in range(U5):
            t = (i * U5 + u) * 2
            b0, b1 = load(b_ref, 0, t), load(b_ref, 1, t)
            p0, p1 = potential(0, t), potential(1, t)
            a0, a1 = load(a_ref, 2 * c, t), load(a_ref, 2 * c + 1, t)
            store(va, 0, t, -(b0 * p0 + b1 * p1))
            p2, p3 = potential(2, t), potential(3, t)
            store(va, 1, t, -(b0 * p2 + b1 * p3))
            store(ob, 0, t, -(a0 * p0 + a1 * p2))
            store(ob, 1, t, -(a0 * p1 + a1 * p3))
        return 0

    def backward_own(i, _):
        for u in range(U5):
            t = (i * U5 + u) * 2
            total = load(va, xl, t)
            for j in range(4):
                total = total - load(a_ref, j, t) * potential(4 + j, t)
            store(va, xl, t, total)
        return 0

    def to_far(e):
        return remote(send, recv, e, va.at[e, theirs, :], back1.at[e], across)

    def to_core(e):
        return remote(send, recv, 2 + e, va.at[e, slab(near), :], back2.at[e], core)

    def to_diagonal(e):
        return remote(send, recv, 4 + e, va.at[e, slab(3 - g), :], back3.at[e], diagonal)

    def owed(j):
        return remote(send, recv, 6 + j, sums.at[j], owed3.at[xl], at((b + 31) % 32, 2 * j + c), 6 + xl)

    def hand_out(e):
        to_far(e).start()
        to_diagonal(e).start()
        to_core(e).start()

    def twofold(n):
        return first_tile(n + 1) - first_tile(n) == 2

    def spread(k, e, rows):
        n = (m + k) % 16
        source = vec.at[e, :, pl.ds(pl.multiple_of(8 * first_tile(n), 8), rows), :]
        target = vc.at[m, e, :, pl.ds(0, rows), :]
        return remote(vsend, vrecv, 16 * e + k, source, target, at(2 * n + xh, g))

    def either(flag, act):
        @pl.when(flag)
        def _():
            act(16)

        @pl.when(jnp.logical_not(flag))
        def _():
            act(8)

    def collect(e):
        for copy_of in (to_far, to_core, to_diagonal):
            copy_of(e).wait_recv()
        vec[e, c] = va[e, mine, :] + back1[e] + owed3[c, e]
        vec[e, 1 - c] = back2[e] + back3[e] + owed3[1 - c, e]

        def start(k, _):
            either(twofold((m + k) % 16), lambda rows: spread(k, e, rows).start())
            return 0

        lax.fori_loop(1, 16, start, 0)
        vc[m, e] = vec[e, :, pl.ds(pl.multiple_of(8 * first_tile(m), 8), 16), :]

    def spread_wait(e):
        def wait(k, _):
            either(twofold((m + k) % 16), lambda rows: spread(k, e, rows).wait_send())
            either(twofold(m), lambda rows: spread(k, e, rows).wait_recv())
            return 0

        lax.fori_loop(1, 16, wait, 0)

    with jax.named_scope("backward_below"):
        lax.fori_loop(0, 9 // U5, backward_below, 0)
        d0 = copy(8, ob.at[:, slab(1 - c), :], owed1.at[0], core)
        d1 = copy(9, ob.at[:, slab(3 - c), :], owed1.at[1], core)
        d0.start()
        d1.start()
        hand_out(1 - xl)
    with jax.named_scope("backward_own"):
        lax.fori_loop(0, 9 // U5, backward_own, 0)
    with jax.named_scope("reduce_owed"):
        d0.wait_recv()
        sums[0] = ob[:, slab(c), :] + owed1[0]
        owed(0).start()
        d1.wait_recv()
        sums[1] = ob[:, slab(2 + c), :] + owed1[1]
        owed(1).start()
        hand_out(xl)
        for sent in (*a_across, a_core, *a_far, b_near, b_wide, b_core, b_far):
            sent.wait_send()
        for j in range(2):
            remote(send, recv, 6 + j, sums.at[j], owed3.at[j], down, 6 + j).wait_recv()
    with jax.named_scope("collect_first"):
        collect(xl)
    with jax.named_scope("collect_last"):
        collect(1 - xl)
    with jax.named_scope("spread_first"):
        for e in range(2):
            for n in range(2):
                v_out[pl.ds(2 * n + e, SLAB, stride=4), :] = vec[e, n]
        for e in range(2):
            for copy_of in (to_far, to_core, to_diagonal):
                copy_of(e).wait_send()
        for sent in (d0, d1, owed(0), owed(1)):
            sent.wait_send()
        o_twin.wait_send()
        first(9, o_all.at[:, xh], o_all.at[:, 1 - xh], twin).wait_recv()
        spread_wait(xl)
    with jax.named_scope("spread_last"):
        spread_wait(1 - xl)

    with jax.named_scope("products"):
        dims = (((1,), (1,)), ((), ()))
        o_rows, v_rows = o_all.reshape(2048, 128), vc.reshape(1024, 128)
        total = jnp.zeros((64, 128), F32)
        for r in range(16):
            some = v_rows[pl.ds(r, 64, stride=16), :]
            if r >= 8:
                some = jnp.where(twofold(m), some, 0.0)
            oh, ol = split(o_rows[pl.ds(r, 128, stride=16), :])
            vh, vl = split(some)
            left = jnp.concatenate([vh, vl, vh], axis=1)
            right = jnp.concatenate([oh, oh, ol], axis=1)
            total = total + lax.dot_general(left, right, dims, preferred_element_type=F32)
        total = total * (1.0 / NCELL)
        lane = lax.broadcasted_iota(jnp.int32, (16, 128), 1) // 32
        slots = (0, 2, 1, 3)
        kinds = [jnp.concatenate([total[4 * n + k : 4 * n + k + 1] for n in range(16)], axis=0) for k in slots]
        for q in range(4):
            row = kinds[q]
            for k in range(4):
                if k != q:
                    row = jnp.where(lane == k, pltpu.roll(kinds[k], 32 * ((k - q) % 4), 1), row)
            part[q] = row

    with jax.named_scope("deal_group"):
        others = [
            remote(nsend, nrecv, k, part.at[(g + k) % 4], near_part.at[k], at(b, (g + k) % 4)) for k in range(1, 4)
        ]
        for sent in others:
            sent.start()
        for sent in others:
            sent.wait()
        group_sum = part[g] + near_part[1] + near_part[2] + near_part[3]
        for n in range(16):
            rows_out[n] = group_sum[n : n + 1, :]

    def deal(k):
        n = (m + k) % 16
        return remote(psend, precv, k, rows_out.at[n], rows_in.at[k], at(2 * n + xh, g))

    def deal_start(k, _):
        deal(k).start()
        return 0

    def deal_wait(k, total):
        deal(k).wait()
        return total + rows_in[k]

    with jax.named_scope("deal"):
        lax.fori_loop(1, 16, deal_start, 0)
        whole = lax.fori_loop(1, 16, deal_wait, rows_out[m])
        for k in range(4):
            m_out[k : k + 1, :] = whole[:, 32 * k : 32 * (k + 1)]


def on_device(orbitals):
    shape = jax.ShapeDtypeStruct
    dma = pltpu.SemaphoreType.DMA

    def room(*dims):
        return pltpu.VMEM(dims, F32)

    packed = orbitals.reshape(4, SLAB, 128).transpose(1, 0, 2).reshape(4 * SLAB, 128)
    half = room(2, 2, SLAB, 128)
    vectors, margin = pl.pallas_call(
        exchange_kernel,
        out_shape=(shape((4 * SLAB, 128), F32), shape((4, 32), F32)),
        in_specs=[pl.BlockSpec(memory_space=pltpu.HBM)] * 2,
        out_specs=(VMEM, VMEM),
        scratch_shapes=[
            room(4 * SLAB, 128), pltpu.VMEM((NG, 3 * NG), BF16), dma((2,)), room(4, 864, 128), room(2, 864, 128),
            room(16, 2, 4, 16, 128), room(3, NG * NG, 128), room(18, 384, 128), room(3, NG * PITCH, 128),
            room(3, NG * PITCH, 128), room(2, 864, 128), room(2, 864, 128), half, half, half,
            room(2, SLAB, 128), room(2, SLAB, 128), room(2, SLAB, 128), half, room(16, 2, 2, 16, 128),
            room(4, 16, 128), room(4, 16, 128), room(16, 1, 128), room(16, 1, 128),
            dma((10,)), dma((10,)), dma((16,)), dma((16,)), dma((10,)), dma((10,)),
            dma((32,)), dma((32,)), dma((16,)), dma((16,)), dma((4,)), dma((4,)),
        ],
        compiler_params=pltpu.CompilerParams(
            collective_id=0, has_side_effects=True, vmem_limit_bytes=67043328
        ),
        name="exchange",
    )(packed, hartley_rows())
    vectors = vectors.reshape(SLAB, 4, 128).transpose(1, 0, 2).reshape(4, SLAB * 128)
    return vectors, margin.T


def solution(mesh):
    return jax.shard_map(
        on_device,
        mesh=mesh,
        in_specs=(P("band", "grid"),),
        out_specs=(P("band", "grid"), P("grid", "band")),
        check_vma=False,
    )
```

```python
import jax
import jax.numpy as jnp
import numpy as np
from jax import lax
from jax.experimental import pallas as pl
from jax.experimental.pallas import tpu as pltpu
from jax.sharding import PartitionSpec as P

NG = 48
NCELL = 110592
PITCH = 52
SLAB = 216
MESH = pl.DeviceIdType.MESH
F32 = jnp.float32
BF16 = jnp.bfloat16
CHUNKS, TILES, SPAN = 3, 6, 72
U3 = 16
VMEM = pl.BlockSpec(memory_space=pltpu.VMEM)


def hartley_rows():
    index = np.arange(NG)
    angles = (index[:, None] * index[None, :] % NG) * (2 * np.pi / NG)
    table = (np.cos(angles) + np.sin(angles)).astype(np.float32)
    high = table.astype(BF16)
    low = (table - high.astype(np.float32)).astype(BF16)
    return jnp.asarray(np.concatenate([high, high, low], axis=1))


def folded(index):
    return ((index + NG // 2) % NG - NG // 2).astype(F32)


def at(b, g):
    return {"band": b, "grid": g}


def part_rows(g, ch):
    return pl.ds(pl.multiple_of(ch * 4 * SPAN + g * SPAN, 8), SPAN)


def split(value):
    high = value.astype(BF16)
    low = (value - high.astype(F32)).astype(BF16)
    return high, low


def hartley(table, value):
    high, low = split(value)
    stack = jnp.concatenate([high, low, high], axis=0)
    dims = (((1,), (0,)), ((), ()))
    return lax.dot_general(table, stack, dims, preferred_element_type=F32)


def fill_kernel(k_ref):
    lane = lax.broadcasted_iota(jnp.int32, (1, 128), 1)
    y = folded(lax.broadcasted_iota(jnp.int32, (NG, 128), 0))
    x = [folded((l * 128 + lane) % NG) for l in range(3)]
    planes = [y * y + v * v for v in x]

    def plane(z, _):
        depth = z.astype(F32)
        depth = depth * depth
        for l in range(3):
            square = planes[l] + depth
            safe = jnp.where(square > 0, square, 1.0)
            value = (40.0 / NCELL) * (1.0 - jnp.exp(-square / 16.0)) / safe
            value = jnp.where(square > 0, value, 0.0)
            k_ref[l, pl.ds(pl.multiple_of(z * NG, 8), NG), :] = value
        return 0

    lax.fori_loop(0, NG // 2 + 1, plane, 0)

    def mirror(z, _):
        for l in range(3):
            source = pl.ds(pl.multiple_of((NG - z) * NG, 8), NG)
            k_ref[l, pl.ds(pl.multiple_of(z * NG, 8), NG), :] = k_ref[l, source, :]
        return 0

    lax.fori_loop(NG // 2 + 1, NG, mirror, 0)


def exchange_kernel(orb_hbm, h_hbm, v_out, m_out, orb, h_ref, load_sem, own, low, a_ref, b_ref, o_all, k_ref, s_ref, r_ref, q_ref,
                    va, ob, owed1, sums, owed3, back1, back2, back3, vec, vc, part, near_part, rows_out, rows_in,
                    gsend, grecv, osend, orecv, send, recv, vsend, vrecv, psend, precv, nsend, nrecv):
    b, g = lax.axis_index("band"), lax.axis_index("grid")
    m, xh, xl, c = b // 2, b % 2, g // 2, g % 2
    far, near = (g + 2) % 4, g + 1 - 2 * c
    across, core, diagonal = at(b, far), at(b, near), at(b, 3 - g)
    up, up_far = at((b + 1) % 32, g), at((b + 1) % 32, far)
    down, down_far = at((b + 31) % 32, g), at((b + 31) % 32, far)
    low_m = (m + 15 + xh) % 16
    fetch = pltpu.make_async_copy(orb_hbm, orb, load_sem.at[0])
    fetch.start()
    fetch_table = pltpu.make_async_copy(h_hbm, h_ref, load_sem.at[1])
    fetch_table.start()
    barrier = pltpu.get_barrier_semaphore()
    for peer in (up, up_far, down, down_far, across, core, diagonal):
        pl.semaphore_signal(barrier, inc=1, device_id=peer, device_id_type=MESH)

    def greet(k, _):
        peer = at(2 * ((m + k) % 16) + xh, g)
        pl.semaphore_signal(barrier, inc=1, device_id=peer, device_id_type=MESH)
        return 0

    lax.fori_loop(1, 16, greet, 0)
    fetch.wait()
    for n in range(4):
        for t in range(18):
            ch, tile = divmod(t, TILES)
            own[n, pl.ds(ch * SPAN + tile, 12, stride=TILES), :] = orb[pl.ds(4 * t + n, 12, stride=72), :]
    for ch in range(CHUNKS):
        a_ref[:, part_rows(g, ch), :] = own[:, ch * SPAN : (ch + 1) * SPAN, :]
    pl.semaphore_wait(barrier, 22)

    def remote(sends, recvs, sem, recv_sem, src, dst, peer):
        return pltpu.make_async_remote_copy(
            src_ref=src, dst_ref=dst, send_sem=sends.at[sem], recv_sem=recvs.at[recv_sem],
            device_id=peer, device_id_type=MESH,
        )

    def first(kind, ch, src, dst, peer):
        return remote(gsend, grecv, kind, CHUNKS * kind + ch, src, dst, peer)

    def same(kind, ch, ref, owner, peer):
        where = ref.at[:, part_rows(owner, ch), :]
        return first(kind, ch, where, where, peer)

    def a_across(ch):
        return same(0, ch, a_ref, g, across)

    def b_wide(ch):
        src = a_ref.at[pl.ds(2 * xl, 2), part_rows(g, ch), :]
        return first(1, ch, src, b_ref.at[:, part_rows(g, ch), :], up)

    def b_near(ch):
        src = a_ref.at[pl.ds(2 - 2 * xl, 2), part_rows(g, ch), :]
        return first(2, ch, src, b_ref.at[:, part_rows(g, ch), :], up_far)

    def a_core(ch):
        return same(3, ch, a_ref, g, core)

    def a_far(ch):
        return same(4, ch, a_ref, far, core)

    def b_core(ch):
        return same(5, ch, b_ref, far, core)

    def b_far(ch):
        return same(6, ch, b_ref, g, core)

    def low_across(ch):
        target = low.at[pl.ds(2 * xl, 2), pl.ds(ch * SPAN, SPAN), :]
        return first(7, ch, b_ref.at[:, part_rows(far, ch), :], target, across)

    def low_in(ch):
        target = low.at[pl.ds(2 - 2 * xl, 2), pl.ds(ch * SPAN, SPAN), :]
        return first(7, ch, b_ref.at[:, part_rows(far, ch), :], target, across)

    a_whole, b_whole, b_half = a_ref.at[:, 0:SLAB, :], b_ref.at[:, 0:SLAB, :], a_ref.at[0:2, 0:SLAB, :]
    gathers = [first(kind, 0, w, w, across) for kind, w in enumerate((a_whole, b_half, b_half, a_whole, a_whole, b_whole, b_whole, b_whole))]

    def tile_rows(tile):
        return pl.ds(pl.multiple_of(8 * tile, 8), 8)

    def other(k, slot, source, block, half, which):
        n = (m + k) % 16
        tile = jnp.where(n <= 10, n + 16, n) if slot else n
        target = o_all.at[block, half, :, pl.ds(8 * slot, 8), :]
        return remote(osend, orecv, which, which, source.at[:, tile_rows(tile), :], target, at(2 * n + xh, g))

    def scatter(source, block, half, which):
        def start(k, _):
            other(k, 0, source, block, half, which).start()
            other(k, 1, source, block, half, which).start()
            return 0

        lax.fori_loop(1, 16, start, 0)
        o_all[block, half, :, 0:8, :] = source[:, tile_rows(m), :]
        o_all[block, half, :, 8:16, :] = source[:, tile_rows(jnp.where(m <= 10, m + 16, m)), :]

    def scattered(which):
        window = o_all.at[0:15, 0]
        remote(osend, orecv, which, which, window, window, across).wait()

    d = 2 * c + xl

    def rows(ch, tile):
        return pl.ds(ch * 4 * SPAN + tile, NG, stride=TILES)

    def load(ref, i, ch, tile):
        return jnp.concatenate([ref[i, rows(ch, tile), :], ref[i, rows(ch, tile + 1), :]], axis=1)

    def store(ref, j, ch, tile, value):
        ref[j, rows(ch, tile), :] = value[:, :128]
        ref[j, rows(ch, tile + 1), :] = value[:, 128:]

    def forward(ch):
        for tile in range(0, TILES, 2):
            t = ch * TILES + tile
            single = load(a_ref, d, ch, tile)
            a0, a1 = load(a_ref, 2 * c, ch, tile), load(a_ref, 2 * c + 1, ch, tile)
            b0, b1 = load(b_ref, 0, ch, tile), load(b_ref, 1, ch, tile)
            for f in range(8):
                left = (a0, a0, a1, a1)[f] if f < 4 else single
                right = (b0, b1, b0, b1)[f] if f < 4 else load(a_ref, f - 4, ch, tile)
                out = hartley(table, left * right)
                s_ref[t, f * 48 : (f + 1) * 48, :] = out[:, :128]
                s_ref[t + 1, f * 48 : (f + 1) * 48, :] = out[:, 128:]

    def block_of(n, i):
        y, z = divmod(n * 8, 48)
        return pl.ds((i * 8 + y) * PITCH + z, 8)

    def turn_in(ch):
        def step(i, _):
            for v in range(3):
                for l in range(3):
                    block = s_ref[i * 3 + v, l * 128 : (l + 1) * 128, :].T
                    for n in range(16):
                        r_ref[l, block_of(v * 16 + n, i), :] = block[n * 8 : (n + 1) * 8, :]
            return 0

        lax.fori_loop(2 * ch, 2 * ch + 2, step, 0)

    def turn_out(ch):
        def step(i, _):
            for v in range(3):
                for l in range(3):
                    parts = [r_ref[l, block_of(v * 16 + n, i), :] for n in range(16)]
                    s_ref[i * 3 + v, l * 128 : (l + 1) * 128, :] = jnp.concatenate(parts, axis=0).T
            return 0

        lax.fori_loop(2 * ch, 2 * ch + 2, step, 0)

    def passes(source, target, where, count, scale=None):
        tiles = [(u, l) for u in range(count) for l in range(3)]
        for p in range(0, len(tiles), 2):
            pair = tiles[p : p + 2]
            value = jnp.concatenate([source[l, where(u), :] for u, l in pair], axis=1)
            out = hartley(table, value)
            for j, (u, l) in enumerate(pair):
                piece = out[:, 128 * j : 128 * (j + 1)]
                if scale is not None:
                    piece = piece * k_ref[l, scale(u), :]
                target[l, where(u), :] = piece

    def along_z(ch, source, target):
        passes(source, target, lambda u: pl.ds((16 * ch + u) * PITCH, 48), 16)

    def along_y(source, target, scaled):
        def step(i, _):
            passes(source, target, lambda u: pl.ds(i * U3 + u, 48, stride=PITCH), U3,
                   (lambda u: pl.ds(pl.multiple_of((i * U3 + u) * 48, 8), 48)) if scaled else None)
            return 0

        lax.fori_loop(0, 48 // U3, step, 0)

    with jax.named_scope("start"):
        for ch in range(CHUNKS):
            for copy_of in (a_across, b_wide, b_near, a_core):
                copy_of(ch).start()
        scatter(own, m, xh, 0)
        fill_kernel(k_ref)
        fetch_table.wait()
    table = h_ref[...]
    for ch in range(CHUNKS):
        with jax.named_scope("gather"):
            b_near(ch).wait_recv()
            b_core(ch).start()
            a_across(ch).wait_recv()
            a_far(ch).start()
            b_wide(ch).wait_recv()
            b_far(ch).start()
            for copy_of in (a_core, b_core, a_far, b_far):
                copy_of(ch).wait_recv()
            if ch == CHUNKS - 1:
                for early in range(CHUNKS):
                    low_across(early).start()
        with jax.named_scope("forward"):
            forward(ch)
        with jax.named_scope("turn_in"):
            turn_in(ch)
        with jax.named_scope("along_z"):
            along_z(ch, r_ref, q_ref)
    with jax.named_scope("along_y"):
        along_y(q_ref, r_ref, True)
    with jax.named_scope("along_y"):
        along_y(r_ref, q_ref, False)

    def potential(f, t):
        span = slice(f * 48, (f + 1) * 48)
        return hartley(table, jnp.concatenate([s_ref[t, span, :], s_ref[t + 1, span, :]], axis=1))

    def backward(ch):
        for tile in range(0, TILES, 2):
            t = ch * TILES + tile
            b0, b1 = load(b_ref, 0, ch, tile), load(b_ref, 1, ch, tile)
            a0, a1 = load(a_ref, 2 * c, ch, tile), load(a_ref, 2 * c + 1, ch, tile)
            p0, p1 = potential(0, t), potential(1, t)
            v0 = b0 * p0 + b1 * p1
            w0, w1 = a0 * p0, a0 * p1
            p2, p3 = potential(2, t), potential(3, t)
            v1 = b0 * p2 + b1 * p3
            store(ob, 0, ch, tile, -(w0 + a1 * p2))
            store(ob, 1, ch, tile, -(w1 + a1 * p3))
            extra = load(a_ref, 0, ch, tile) * potential(4, t)
            for j in range(1, 4):
                extra = extra + load(a_ref, j, ch, tile) * potential(4 + j, t)
            store(va, 0, ch, tile, -(v0 + jnp.where(xl == 0, extra, 0.0)))
            store(va, 1, ch, tile, -(v1 + jnp.where(xl == 0, 0.0, extra)))

    def second(kind, ch, src, dst, peer, recv_kind=None):
        recv_at = CHUNKS * (kind if recv_kind is None else recv_kind) + ch
        return remote(send, recv, kind, recv_at, src, dst, peer)

    def to_far(ch):
        return second(0, ch, va.at[:, part_rows(far, ch), :], back1.at[ch], across)

    def to_core(ch):
        return second(1, ch, va.at[:, part_rows(near, ch), :], back2.at[ch], core)

    def to_diagonal(ch):
        return second(2, ch, va.at[:, part_rows(3 - g, ch), :], back3.at[ch], diagonal)

    def owed_core(j, ch):
        return second(3 + j, ch, ob.at[:, part_rows(2 * j + 1 - c, ch), :], owed1.at[ch, j], core)

    def owed(j, ch):
        return second(5 + j, ch, sums.at[ch, j], owed3.at[ch, xl], at((b + 31) % 32, 2 * j + c), 5 + xl)

    def owed_in(j, ch):
        return second(5 + j, ch, sums.at[ch, j], owed3.at[ch, j], down)

    def hand_out(ch):
        owed_core(0, ch).start()
        owed_core(1, ch).start()
        to_far(ch).start()
        to_diagonal(ch).start()
        to_core(ch).start()

    def pass_owed(ch):
        for j in range(2):
            owed_core(j, ch).wait_recv()
            sums[ch, j] = ob[:, part_rows(2 * j + c, ch), :] + owed1[ch, j]
            owed(j, ch).start()

    def spread(ch, j):
        tile = 9 * ch + j
        n, slot = tile % 16, tile // 16
        source = vec.at[:, :, tile_rows(tile), :]
        target = vc.at[m, :, :, pl.ds(pl.multiple_of(8 * slot, 8), 8), :]
        return remote(vsend, vrecv, 0, 0, source, target, at(2 * n + xh, g)), n

    def spread_done(sent, got):
        window = vec.at[:, :, pl.ds(0, 8 * sent), :]
        remote(vsend, vrecv, 0, 0, window, window, across).wait_send()
        window = vc.at[0:15, :, :, pl.ds(0, got), :]
        remote(vsend, vrecv, 0, 0, window, window, across).wait_recv()

    def collect(ch):
        for copy_of in (to_far, to_core, to_diagonal):
            copy_of(ch).wait_recv()
        for j in range(2):
            owed_in(j, ch).wait_recv()
        where = pl.ds(ch * SPAN, SPAN)
        for e in range(2):
            vec[e, c, where, :] = va[e, part_rows(g, ch), :] + back1[ch, e] + owed3[ch, c, e]
            vec[e, 1 - c, where, :] = back2[ch, e] + back3[ch, e] + owed3[ch, 1 - c, e]

        def start(k, _):
            copy, n = spread(ch, (k + m) % 9)

            @pl.when(n != m)
            def _():
                copy.start()

            return 0

        lax.fori_loop(0, 9, start, 0)
        for t in range(TILES * ch, TILES * ch + TILES):
            place = pl.ds(ch * SPAN + t % TILES, 12, stride=TILES)
            for e in range(2):
                for n in range(2):
                    v_out[pl.ds(4 * t + 2 * n + e, 12, stride=72), :] = vec[e, n, place, :]

    for ch in range(CHUNKS):
        with jax.named_scope("along_z"):
            along_z(ch, q_ref, r_ref)
        with jax.named_scope("turn_out"):
            turn_out(ch)
        if ch > 0:
            with jax.named_scope("pass_owed"):
                pass_owed(ch - 1)
        with jax.named_scope("backward"):
            backward(ch)
            hand_out(ch)
    with jax.named_scope("pass_owed"):
        pass_owed(CHUNKS - 1)
    with jax.named_scope("low"):
        for sent in gathers:
            sent.wait_send()
        for ch in range(CHUNKS):
            low_in(ch).wait_recv()
            low[pl.ds(2 * xl, 2), pl.ds(ch * SPAN, SPAN), :] = b_ref[:, part_rows(g, ch), :]
        scatter(low, low_m, 1 - xh, 1)
    for ch in range(CHUNKS):
        with jax.named_scope("collect"):
            collect(ch)
    with jax.named_scope("spread_wait"):
        vc[m, :, :, 0:8, :] = vec[:, :, tile_rows(m), :]
        vc[m, :, :, 8:16, :] = vec[:, :, tile_rows(jnp.where(m <= 10, m + 16, m)), :]
        for kind, w in enumerate((va, va, va, ob, ob, sums, sums)):
            if kind < 5:
                whole = w.at[:, 0:SLAB, :]
            else:
                whole = w.at[:, 0]
            remote(send, recv, kind, kind, whole, whole, across).wait_send()
        scattered(0)
        scattered(1)

        @pl.when(m <= 10)
        def _():
            spread_done(25, 16)

        @pl.when(m > 10)
        def _():
            spread_done(26, 8)

    with jax.named_scope("products"):
        dims = (((1,), (1,)), ((), ()))
        o_rows, v_rows = o_all.reshape(2048, 128), vc.reshape(1024, 128)
        total = jnp.zeros((64, 128), F32)
        for r in range(16):
            some = v_rows[pl.ds(r, 64, stride=16), :]
            if r >= 8:
                some = jnp.where(m <= 10, some, 0.0)
            oh, ol = split(o_rows[pl.ds(r, 128, stride=16), :])
            vh, vl = split(some)
            left = jnp.concatenate([vh, vl, vh], axis=1)
            right = jnp.concatenate([oh, oh, ol], axis=1)
            total = total + lax.dot_general(left, right, dims, preferred_element_type=F32)
        total = total * (1.0 / NCELL)
        lane = lax.broadcasted_iota(jnp.int32, (16, 128), 1) // 32
        slots = (0, 2, 1, 3)
        kinds = [jnp.concatenate([total[4 * n + k : 4 * n + k + 1] for n in range(16)], axis=0) for k in slots]
        for q in range(4):
            row = kinds[q]
            for k in range(4):
                if k != q:
                    row = jnp.where(lane == k, pltpu.roll(kinds[k], 32 * ((k - q) % 4), 1), row)
            part[q] = row

    with jax.named_scope("deal_group"):
        for k in range(1, 4):
            remote(nsend, nrecv, 0, 0, part.at[(g + k) % 4], near_part.at[k], at(b, (g + k) % 4)).start()
        window = near_part.at[1:4]
        remote(nsend, nrecv, 0, 0, window, window, across).wait()
        group_sum = part[g] + near_part[1] + near_part[2] + near_part[3]
        for n in range(16):
            rows_out[n] = group_sum[n : n + 1, :]

    def deal_start(k, _):
        n = (m + k) % 16
        remote(psend, precv, 0, 0, rows_out.at[n], rows_in.at[k], at(2 * n + xh, g)).start()
        return 0

    with jax.named_scope("deal"):
        lax.fori_loop(1, 16, deal_start, 0)
        window = rows_in.at[1:16]
        remote(psend, precv, 0, 0, window, window, across).wait()
        whole = rows_out[m]
        for k in range(1, 16):
            whole = whole + rows_in[k]
        for k in range(4):
            m_out[k : k + 1, :] = whole[:, 32 * k : 32 * (k + 1)]


def on_device(orbitals):
    shape = jax.ShapeDtypeStruct
    dma = pltpu.SemaphoreType.DMA

    def room(*dims):
        return pltpu.VMEM(dims, F32)

    packed = orbitals.reshape(4, SLAB, 128).transpose(1, 0, 2).reshape(4 * SLAB, 128)
    triple = room(CHUNKS, 2, SPAN, 128)
    pairs = room(CHUNKS, 2, 2, SPAN, 128)
    vectors, margin = pl.pallas_call(
        exchange_kernel,
        out_shape=(pltpu.VMEM((4 * SLAB, 128), F32), pltpu.VMEM((4, 32), F32)),
        in_specs=[pl.BlockSpec(memory_space=pltpu.HBM)] * 2,
        out_specs=(VMEM, VMEM),
        scratch_shapes=[
            room(4 * SLAB, 128), pltpu.VMEM((NG, 3 * NG), BF16), dma((2,)), room(4, SLAB, 128), room(4, SLAB, 128),
            room(4, 864, 128), room(2, 864, 128), room(16, 2, 4, 16, 128), room(3, NG * NG, 128),
            room(18, 384, 128), room(3, NG * PITCH, 128), room(3, NG * PITCH, 128),
            room(2, 864, 128), room(2, 864, 128), pairs, pairs, pairs, triple, triple, triple,
            room(2, 2, SLAB, 128), room(16, 2, 2, 16, 128),
            room(4, 16, 128), room(4, 16, 128), room(16, 1, 128), room(16, 1, 128),
            dma((8,)), dma((24,)), dma((2,)), dma((2,)), dma((7,)), dma((21,)),
            dma((1,)), dma((1,)), dma((1,)), dma((1,)), dma((1,)), dma((1,)),
        ],
        compiler_params=pltpu.CompilerParams(
            collective_id=0, has_side_effects=True, vmem_limit_bytes=56 * 1024 * 1024
        ),
        name="exchange",
    )(
        pltpu.with_memory_space_constraint(packed, pltpu.HBM),
        pltpu.with_memory_space_constraint(hartley_rows(), pltpu.HBM),
    )
    vectors = vectors.reshape(SLAB, 4, 128).transpose(1, 0, 2).reshape(4, SLAB * 128)
    return vectors, margin.T


def solution(mesh):
    return jax.shard_map(
        on_device,
        mesh=mesh,
        in_specs=(P("band", "grid"),),
        out_specs=(P("band", "grid"), P("grid", "band")),
        check_vma=False,
    )
```

```python
import jax
import jax.numpy as jnp
import numpy as np
from jax import lax
from jax.experimental import pallas as pl
from jax.experimental.pallas import tpu as pltpu
from jax.sharding import PartitionSpec as P

NG = 48
NCELL = 110592
PITCH = 52
SLAB = 216
MESH = pl.DeviceIdType.MESH
F32 = jnp.float32
BF16 = jnp.bfloat16
CHUNKS, TILES, SPAN = 3, 6, 72
U3 = 16
VMEM = pl.BlockSpec(memory_space=pltpu.VMEM)


def hartley_rows():
    index = np.arange(NG)
    angles = (index[:, None] * index[None, :] % NG) * (2 * np.pi / NG)
    table = (np.cos(angles) + np.sin(angles)).astype(np.float32)
    high = table.astype(BF16)
    low = (table - high.astype(np.float32)).astype(BF16)
    return jnp.asarray(np.concatenate([high, high, low], axis=1))


def folded(index):
    return ((index + NG // 2) % NG - NG // 2).astype(F32)


def at(b, g):
    return {"band": b, "grid": g}


def part_rows(g, ch):
    return pl.ds(pl.multiple_of(ch * 4 * SPAN + g * SPAN, 8), SPAN)


def split(value):
    high = value.astype(BF16)
    low = (value - high.astype(F32)).astype(BF16)
    return high, low


def hartley(table, value):
    high, low = split(value)
    stack = jnp.concatenate([high, low, high], axis=0)
    dims = (((1,), (0,)), ((), ()))
    return lax.dot_general(table, stack, dims, preferred_element_type=F32)


def fill_kernel(k_ref):
    lane = lax.broadcasted_iota(jnp.int32, (1, 128), 1)
    y = folded(lax.broadcasted_iota(jnp.int32, (NG, 128), 0))
    x = [folded((l * 128 + lane) % NG) for l in range(3)]
    planes = [y * y + v * v for v in x]

    def plane(z, _):
        depth = z.astype(F32)
        depth = depth * depth
        for l in range(3):
            square = planes[l] + depth
            safe = jnp.where(square > 0, square, 1.0)
            value = (40.0 / NCELL) * (1.0 - jnp.exp(-square / 16.0)) / safe
            value = jnp.where(square > 0, value, 0.0)
            k_ref[l, pl.ds(pl.multiple_of(z * NG, 8), NG), :] = value
        return 0

    lax.fori_loop(0, NG // 2 + 1, plane, 0)

    def mirror(z, _):
        for l in range(3):
            source = pl.ds(pl.multiple_of((NG - z) * NG, 8), NG)
            k_ref[l, pl.ds(pl.multiple_of(z * NG, 8), NG), :] = k_ref[l, source, :]
        return 0

    lax.fori_loop(NG // 2 + 1, NG, mirror, 0)


def exchange_kernel(orb_hbm, h_hbm, v_out, m_out, orb, h_ref, load_sem, own, low, a_ref, b_ref, o_all, k_ref, s_ref, r_ref, q_ref,
                    va, ob, owed1, sums, owed3, back1, back2, back3, vec, vc, summed, part, rows_in,
                    gsend, grecv, osend, orecv, send, recv, vsend, vrecv, psend, precv):
    b, g = lax.axis_index("band"), lax.axis_index("grid")
    m, xh, xl, c = b // 2, b % 2, g // 2, g % 2
    far, near = (g + 2) % 4, g + 1 - 2 * c
    across, core, diagonal = at(b, far), at(b, near), at(b, 3 - g)
    up, up_far = at((b + 1) % 32, g), at((b + 1) % 32, far)
    down, down_far = at((b + 31) % 32, g), at((b + 31) % 32, far)
    low_m = (m + 15 + xh) % 16
    fetch = pltpu.make_async_copy(orb_hbm, orb, load_sem.at[0])
    fetch.start()
    fetch_table = pltpu.make_async_copy(h_hbm, h_ref, load_sem.at[1])
    fetch_table.start()
    barrier = pltpu.get_barrier_semaphore()
    for peer in (up, up_far, down, down_far, across, core, diagonal):
        pl.semaphore_signal(barrier, inc=1, device_id=peer, device_id_type=MESH)

    def greet(k, _):
        peer = at(2 * ((m + k) % 16) + xh, g)
        pl.semaphore_signal(barrier, inc=1, device_id=peer, device_id_type=MESH)
        return 0

    lax.fori_loop(1, 16, greet, 0)
    fetch.wait()
    for n in range(4):
        for t in range(18):
            ch, tile = divmod(t, TILES)
            own[n, pl.ds(ch * SPAN + tile, 12, stride=TILES), :] = orb[pl.ds(4 * t + n, 12, stride=72), :]
    for ch in range(CHUNKS):
        a_ref[:, part_rows(g, ch), :] = own[:, ch * SPAN : (ch + 1) * SPAN, :]
    pl.semaphore_wait(barrier, 22)

    def remote(sends, recvs, sem, recv_sem, src, dst, peer):
        return pltpu.make_async_remote_copy(
            src_ref=src, dst_ref=dst, send_sem=sends.at[sem], recv_sem=recvs.at[recv_sem],
            device_id=peer, device_id_type=MESH,
        )

    def first(kind, ch, src, dst, peer):
        return remote(gsend, grecv, kind, CHUNKS * kind + ch, src, dst, peer)

    def same(kind, ch, ref, owner, peer):
        where = ref.at[:, part_rows(owner, ch), :]
        return first(kind, ch, where, where, peer)

    def a_across(ch):
        return same(0, ch, a_ref, g, across)

    def b_wide(ch):
        src = a_ref.at[pl.ds(2 * xl, 2), part_rows(g, ch), :]
        return first(1, ch, src, b_ref.at[:, part_rows(g, ch), :], up)

    def b_near(ch):
        src = a_ref.at[pl.ds(2 - 2 * xl, 2), part_rows(g, ch), :]
        return first(2, ch, src, b_ref.at[:, part_rows(g, ch), :], up_far)

    def a_core(ch):
        return same(3, ch, a_ref, g, core)

    def a_far(ch):
        return same(4, ch, a_ref, far, core)

    def b_core(ch):
        return same(5, ch, b_ref, far, core)

    def b_far(ch):
        return same(6, ch, b_ref, g, core)

    def low_across(ch):
        target = low.at[pl.ds(2 * xl, 2), pl.ds(ch * SPAN, SPAN), :]
        return first(7, ch, b_ref.at[:, part_rows(far, ch), :], target, across)

    def low_in(ch):
        target = low.at[pl.ds(2 - 2 * xl, 2), pl.ds(ch * SPAN, SPAN), :]
        return first(7, ch, b_ref.at[:, part_rows(far, ch), :], target, across)

    a_whole, b_whole, b_half = a_ref.at[:, 0:SLAB, :], b_ref.at[:, 0:SLAB, :], a_ref.at[0:2, 0:SLAB, :]
    gathers = [first(kind, 0, w, w, across) for kind, w in enumerate((a_whole, b_half, b_half, a_whole, a_whole, b_whole, b_whole, b_whole))]

    def tile_rows(tile):
        return pl.ds(pl.multiple_of(8 * tile, 8), 8)

    def other(k, slot, source, block, half, which):
        n = (m + k) % 16
        tile = jnp.where(n <= 10, n + 16, n) if slot else n
        target = o_all.at[block, half, :, pl.ds(8 * slot, 8), :]
        return remote(osend, orecv, which, which, source.at[:, tile_rows(tile), :], target, at(2 * n + xh, g))

    def scatter(source, block, half, which):
        def start(k, _):
            other(k, 0, source, block, half, which).start()
            other(k, 1, source, block, half, which).start()
            return 0

        lax.fori_loop(1, 16, start, 0)
        o_all[block, half, :, 0:8, :] = source[:, tile_rows(m), :]
        o_all[block, half, :, 8:16, :] = source[:, tile_rows(jnp.where(m <= 10, m + 16, m)), :]

    def scattered(which):
        window = o_all.at[0:15, 0]
        remote(osend, orecv, which, which, window, window, across).wait()

    d = 2 * c + xl

    def rows(ch, tile):
        return pl.ds(ch * 4 * SPAN + tile, NG, stride=TILES)

    def load(ref, i, ch, tile):
        return jnp.concatenate([ref[i, rows(ch, tile), :], ref[i, rows(ch, tile + 1), :]], axis=1)

    def store(ref, j, ch, tile, value):
        ref[j, rows(ch, tile), :] = value[:, :128]
        ref[j, rows(ch, tile + 1), :] = value[:, 128:]

    def forward(ch):
        for tile in range(0, TILES, 2):
            t = ch * TILES + tile
            single = load(a_ref, d, ch, tile)
            a0, a1 = load(a_ref, 2 * c, ch, tile), load(a_ref, 2 * c + 1, ch, tile)
            b0, b1 = load(b_ref, 0, ch, tile), load(b_ref, 1, ch, tile)
            for f in range(8):
                left = (a0, a0, a1, a1)[f] if f < 4 else single
                right = (b0, b1, b0, b1)[f] if f < 4 else load(a_ref, f - 4, ch, tile)
                out = hartley(table, left * right)
                s_ref[t, f * 48 : (f + 1) * 48, :] = out[:, :128]
                s_ref[t + 1, f * 48 : (f + 1) * 48, :] = out[:, 128:]

    def block_of(n, i):
        y, z = divmod(n * 8, 48)
        return pl.ds((i * 8 + y) * PITCH + z, 8)

    def turn_in(ch):
        def step(i, _):
            for v in range(3):
                for l in range(3):
                    block = s_ref[i * 3 + v, l * 128 : (l + 1) * 128, :].T
                    for n in range(16):
                        r_ref[l, block_of(v * 16 + n, i), :] = block[n * 8 : (n + 1) * 8, :]
            return 0

        lax.fori_loop(2 * ch, 2 * ch + 2, step, 0)

    def turn_out(ch):
        def step(i, _):
            for v in range(3):
                for l in range(3):
                    parts = [r_ref[l, block_of(v * 16 + n, i), :] for n in range(16)]
                    s_ref[i * 3 + v, l * 128 : (l + 1) * 128, :] = jnp.concatenate(parts, axis=0).T
            return 0

        lax.fori_loop(2 * ch, 2 * ch + 2, step, 0)

    def passes(source, target, where, count, scale=None):
        tiles = [(u, l) for u in range(count) for l in range(3)]
        for p in range(0, len(tiles), 2):
            pair = tiles[p : p + 2]
            value = jnp.concatenate([source[l, where(u), :] for u, l in pair], axis=1)
            out = hartley(table, value)
            for j, (u, l) in enumerate(pair):
                piece = out[:, 128 * j : 128 * (j + 1)]
                if scale is not None:
                    piece = piece * k_ref[l, scale(u), :]
                target[l, where(u), :] = piece

    def along_z(ch, source, target):
        passes(source, target, lambda u: pl.ds((16 * ch + u) * PITCH, 48), 16)

    def along_y(source, target, scaled):
        def step(i, _):
            passes(source, target, lambda u: pl.ds(i * U3 + u, 48, stride=PITCH), U3,
                   (lambda u: pl.ds(pl.multiple_of((i * U3 + u) * 48, 8), 48)) if scaled else None)
            return 0

        lax.fori_loop(0, 48 // U3, step, 0)

    with jax.named_scope("start"):
        for ch in range(CHUNKS):
            for copy_of in (b_wide, b_near, a_across, a_core):
                copy_of(ch).start()
        scatter(own, m, xh, 0)
        fill_kernel(k_ref)
        fetch_table.wait()
    table = h_ref[...]
    for ch in range(CHUNKS):
        with jax.named_scope("gather"):
            b_near(ch).wait_recv()
            b_core(ch).start()
            a_across(ch).wait_recv()
            a_far(ch).start()
            b_wide(ch).wait_recv()
            b_far(ch).start()
            for copy_of in (a_core, b_core, a_far, b_far):
                copy_of(ch).wait_recv()
            if ch == CHUNKS - 1:
                for early in range(CHUNKS):
                    low_across(early).start()
        with jax.named_scope("forward"):
            forward(ch)
        with jax.named_scope("turn_in"):
            turn_in(ch)
        with jax.named_scope("along_z"):
            along_z(ch, r_ref, q_ref)
    with jax.named_scope("along_y"):
        along_y(q_ref, r_ref, True)
    with jax.named_scope("along_y"):
        along_y(r_ref, q_ref, False)

    def potential(f, t):
        span = slice(f * 48, (f + 1) * 48)
        return hartley(table, jnp.concatenate([s_ref[t, span, :], s_ref[t + 1, span, :]], axis=1))

    def backward(ch):
        for tile in range(0, TILES, 2):
            t = ch * TILES + tile
            b0, b1 = load(b_ref, 0, ch, tile), load(b_ref, 1, ch, tile)
            a0, a1 = load(a_ref, 2 * c, ch, tile), load(a_ref, 2 * c + 1, ch, tile)
            p0, p1 = potential(0, t), potential(1, t)
            v0 = b0 * p0 + b1 * p1
            w0, w1 = a0 * p0, a0 * p1
            p2, p3 = potential(2, t), potential(3, t)
            v1 = b0 * p2 + b1 * p3
            store(ob, 0, ch, tile, -(w0 + a1 * p2))
            store(ob, 1, ch, tile, -(w1 + a1 * p3))
            extra = load(a_ref, 0, ch, tile) * potential(4, t)
            for j in range(1, 4):
                extra = extra + load(a_ref, j, ch, tile) * potential(4 + j, t)
            store(va, 0, ch, tile, -(v0 + jnp.where(xl == 0, extra, 0.0)))
            store(va, 1, ch, tile, -(v1 + jnp.where(xl == 0, 0.0, extra)))

    def second(kind, ch, src, dst, peer, recv_kind=None):
        recv_at = CHUNKS * (kind if recv_kind is None else recv_kind) + ch
        return remote(send, recv, kind, recv_at, src, dst, peer)

    def to_far(ch):
        return second(0, ch, va.at[:, part_rows(far, ch), :], back1.at[ch], across)

    def to_core(ch):
        return second(1, ch, va.at[:, part_rows(near, ch), :], back2.at[ch], core)

    def to_diagonal(ch):
        return second(2, ch, va.at[:, part_rows(3 - g, ch), :], back3.at[ch], diagonal)

    def owed_core(j, ch):
        return second(3 + j, ch, ob.at[:, part_rows(2 * j + 1 - c, ch), :], owed1.at[ch, j], core)

    def owed(j, ch):
        return second(5 + j, ch, sums.at[ch, j], owed3.at[ch, xl], at((b + 31) % 32, 2 * j + c), 5 + xl)

    def owed_in(j, ch):
        return second(5 + j, ch, sums.at[ch, j], owed3.at[ch, j], down)

    def hand_out(ch):
        owed_core(0, ch).start()
        owed_core(1, ch).start()
        if ch == 0:
            to_far(ch).start()
            to_diagonal(ch).start()
        to_core(ch).start()

    def pass_owed(ch):
        for j in range(2):
            owed_core(j, ch).wait_recv()
            sums[ch, j] = ob[:, part_rows(2 * j + c, ch), :] + owed1[ch, j]
            owed(j, ch).start()
        if ch > 0:
            to_far(ch).start()
            to_diagonal(ch).start()

    def spread(ch, j):
        tile = 9 * ch + j
        n, slot = tile % 16, tile // 16
        source = vec.at[:, :, tile_rows(tile), :]
        target = vc.at[m, :, :, pl.ds(pl.multiple_of(8 * slot, 8), 8), :]
        return remote(vsend, vrecv, 0, slot, source, target, at(2 * n + xh, g)), n

    def spread_sent(count):
        window = vec.at[:, :, pl.ds(0, 8 * count), :]
        remote(vsend, vrecv, 0, 0, window, window, across).wait_send()

    def spread_in(slot):
        window = vc.at[0:15, :, :, pl.ds(8 * slot, 8), :]
        remote(vsend, vrecv, 0, slot, window, window, across).wait_recv()

    def collect(ch):
        for copy_of in (to_far, to_core, to_diagonal):
            copy_of(ch).wait_recv()
        for j in range(2):
            owed_in(j, ch).wait_recv()
        where = pl.ds(ch * SPAN, SPAN)
        for e in range(2):
            vec[e, c, where, :] = va[e, part_rows(g, ch), :] + back1[ch, e] + owed3[ch, c, e]
            vec[e, 1 - c, where, :] = back2[ch, e] + back3[ch, e] + owed3[ch, 1 - c, e]

        def start(k, _):
            copy, n = spread(ch, (k + m) % 9)

            @pl.when(n != m)
            def _():
                copy.start()

            return 0

        lax.fori_loop(0, 9, start, 0)
        for t in range(TILES * ch, TILES * ch + TILES):
            place = pl.ds(ch * SPAN + t % TILES, 12, stride=TILES)
            for e in range(2):
                for n in range(2):
                    v_out[pl.ds(4 * t + 2 * n + e, 12, stride=72), :] = vec[e, n, place, :]

    for ch in range(CHUNKS):
        with jax.named_scope("along_z"):
            along_z(ch, q_ref, r_ref)
        with jax.named_scope("turn_out"):
            turn_out(ch)
        if ch > 0:
            with jax.named_scope("pass_owed"):
                pass_owed(ch - 1)
        with jax.named_scope("backward"):
            backward(ch)
            hand_out(ch)
    with jax.named_scope("pass_owed"):
        pass_owed(CHUNKS - 1)
    with jax.named_scope("low"):
        for sent in gathers:
            sent.wait_send()
        for ch in range(CHUNKS):
            low_in(ch).wait_recv()
            low[pl.ds(2 * xl, 2), pl.ds(ch * SPAN, SPAN), :] = b_ref[:, part_rows(g, ch), :]
        scatter(low, low_m, 1 - xh, 1)
    for ch in range(CHUNKS):
        with jax.named_scope("collect"):
            collect(ch)
    with jax.named_scope("spread_wait"):
        vc[m, :, :, 0:8, :] = vec[:, :, tile_rows(m), :]
        vc[m, :, :, 8:16, :] = vec[:, :, tile_rows(jnp.where(m <= 10, m + 16, m)), :]
        for kind, w in enumerate((va, va, va, ob, ob, sums, sums)):
            if kind < 5:
                whole = w.at[:, 0:SLAB, :]
            else:
                whole = w.at[:, 0]
            remote(send, recv, kind, kind, whole, whole, across).wait_send()
        scattered(0)
        scattered(1)

        spread_in(0)

    dims = (((1,), (1,)), ((), ()))
    o_rows, v_rows = o_all.reshape(2048, 128), vc.reshape(1024, 128)

    def products(start):
        total = jnp.zeros((64, 128), F32)
        for r in range(start, start + 8):
            oh, ol = split(o_rows[pl.ds(r, 128, stride=16), :])
            vh, vl = split(v_rows[pl.ds(r, 64, stride=16), :])
            left = jnp.concatenate([vh, vl, vh], axis=1)
            right = jnp.concatenate([oh, oh, ol], axis=1)
            total = total + lax.dot_general(left, right, dims, preferred_element_type=F32)
        return total

    with jax.named_scope("products_first"):
        summed[...] = products(0)
    with jax.named_scope("spread_last"):

        @pl.when(m <= 10)
        def _():
            spread_in(1)
            summed[...] = summed[...] + products(8)
            spread_sent(25)

        @pl.when(m > 10)
        def _():
            spread_sent(26)

    with jax.named_scope("arrange"):
        total = summed[...]
        total = total * (1.0 / NCELL)
        lane = lax.broadcasted_iota(jnp.int32, (16, 128), 1) // 32
        slots = (0, 2, 1, 3)
        kinds = [jnp.concatenate([total[4 * n + k : 4 * n + k + 1] for n in range(16)], axis=0) for k in slots]
        for q in range(4):
            row = kinds[q]
            for k in range(4):
                if k != q:
                    row = jnp.where(lane == k, pltpu.roll(kinds[k], 32 * ((k - q) % 4), 1), row)
            for n in range(16):
                part[4 * n + q] = row[n : n + 1, :]

    def deal_start(k, _):
        n = (m + k) % 16
        for j in range(4):
            q = (g + j) % 4
            copy = remote(psend, precv, 0, 0, part.at[4 * n + q], rows_in.at[4 * k + j], at(2 * n + xh, q))
            if j > 0:
                copy.start()
            else:
                pl.when(k < 16)(copy.start)
        return 0

    with jax.named_scope("deal"):
        lax.fori_loop(1, 17, deal_start, 0)
        window = rows_in.at[4:67]
        remote(psend, precv, 0, 0, window, window, across).wait()
        whole = part[4 * m + g]
        for k in range(4, 68):
            if k != 64:
                whole = whole + rows_in[k]
        for k in range(4):
            m_out[k : k + 1, :] = whole[:, 32 * k : 32 * (k + 1)]


def on_device(orbitals):
    shape = jax.ShapeDtypeStruct
    dma = pltpu.SemaphoreType.DMA

    def room(*dims):
        return pltpu.VMEM(dims, F32)

    packed = orbitals.reshape(4, SLAB, 128).transpose(1, 0, 2).reshape(4 * SLAB, 128)
    triple = room(CHUNKS, 2, SPAN, 128)
    pairs = room(CHUNKS, 2, 2, SPAN, 128)
    vectors, margin = pl.pallas_call(
        exchange_kernel,
        out_shape=(pltpu.VMEM((4 * SLAB, 128), F32), pltpu.VMEM((4, 32), F32)),
        in_specs=[pl.BlockSpec(memory_space=pltpu.HBM)] * 2,
        out_specs=(VMEM, VMEM),
        scratch_shapes=[
            room(4 * SLAB, 128), pltpu.VMEM((NG, 3 * NG), BF16), dma((2,)), room(4, SLAB, 128), room(4, SLAB, 128),
            room(4, 864, 128), room(2, 864, 128), room(16, 2, 4, 16, 128), room(3, NG * NG, 128),
            room(18, 384, 128), room(3, NG * PITCH, 128), room(3, NG * PITCH, 128),
            room(2, 864, 128), room(2, 864, 128), pairs, pairs, pairs, triple, triple, triple,
            room(2, 2, SLAB, 128), room(16, 2, 2, 16, 128), room(64, 128),
            room(64, 1, 128), room(68, 1, 128),
            dma((8,)), dma((24,)), dma((2,)), dma((2,)), dma((7,)), dma((21,)),
            dma((1,)), dma((2,)), dma((1,)), dma((1,)),
        ],
        compiler_params=pltpu.CompilerParams(
            collective_id=0, has_side_effects=True, vmem_limit_bytes=56 * 1024 * 1024
        ),
        name="exchange",
    )(
        pltpu.with_memory_space_constraint(packed, pltpu.HBM),
        pltpu.with_memory_space_constraint(hartley_rows(), pltpu.HBM),
    )
    vectors = vectors.reshape(SLAB, 4, 128).transpose(1, 0, 2).reshape(4, SLAB * 128)
    return vectors, margin.T


def solution(mesh):
    return jax.shard_map(
        on_device,
        mesh=mesh,
        in_specs=(P("band", "grid"),),
        out_specs=(P("band", "grid"), P("grid", "band")),
        check_vma=False,
    )
```

```python
import jax
import jax.numpy as jnp
import numpy as np
from jax import lax
from jax.experimental import pallas as pl
from jax.experimental.pallas import tpu as pltpu
from jax.sharding import PartitionSpec as P

NG = 48
NCELL = 110592
PITCH = 52
SLAB = 216
MESH = pl.DeviceIdType.MESH
F32 = jnp.float32
BF16 = jnp.bfloat16
CHUNKS, TILES, SPAN = 3, 6, 72
U3 = 48
VMEM = pl.BlockSpec(memory_space=pltpu.VMEM)


def hartley_rows():
    index = np.arange(NG)
    angles = (index[:, None] * index[None, :] % NG) * (2 * np.pi / NG)
    table = (np.cos(angles) + np.sin(angles)).astype(np.float32)
    high = table.astype(BF16)
    low = (table - high.astype(np.float32)).astype(BF16)
    return jnp.asarray(np.concatenate([high, high, low], axis=1))


def folded(index):
    return ((index + NG // 2) % NG - NG // 2).astype(F32)


def at(b, g):
    return {"band": b, "grid": g}


def part_rows(g, ch):
    return pl.ds(pl.multiple_of(ch * 4 * SPAN + g * SPAN, 8), SPAN)


def split(value):
    high = value.astype(BF16)
    low = (value - high.astype(F32)).astype(BF16)
    return high, low


def hartley(table, value):
    high, low = split(value)
    stack = jnp.concatenate([high, low, high], axis=0)
    dims = (((1,), (0,)), ((), ()))
    return lax.dot_general(table, stack, dims, preferred_element_type=F32)


def fill_kernel(k_ref):
    lane = lax.broadcasted_iota(jnp.int32, (1, 128), 1)
    y = folded(lax.broadcasted_iota(jnp.int32, (NG, 128), 0))
    x = [folded((l * 128 + lane) % NG) for l in range(3)]
    planes = [y * y + v * v for v in x]

    def plane(z, _):
        depth = z.astype(F32)
        depth = depth * depth
        for l in range(3):
            square = planes[l] + depth
            safe = jnp.where(square > 0, square, 1.0)
            value = (40.0 / NCELL) * (1.0 - jnp.exp(-square / 16.0)) / safe
            value = jnp.where(square > 0, value, 0.0)
            k_ref[l, pl.ds(pl.multiple_of(z * NG, 8), NG), :] = value
        return 0

    lax.fori_loop(0, NG // 2 + 1, plane, 0)

    def mirror(z, _):
        for l in range(3):
            source = pl.ds(pl.multiple_of((NG - z) * NG, 8), NG)
            k_ref[l, pl.ds(pl.multiple_of(z * NG, 8), NG), :] = k_ref[l, source, :]
        return 0

    lax.fori_loop(NG // 2 + 1, NG, mirror, 0)


def exchange_kernel(orb_hbm, h_hbm, v_out, m_out, orb, h_ref, load_sem, own, low, a_ref, b_ref, o_all, k_ref, s_ref, r_ref, q_ref,
                    va, ob, owed1, sums, owed3, back1, back2, back3, vec, vc, summed, part, rows_in,
                    gsend, grecv, osend, orecv, send, recv, vsend, vrecv, psend, precv):
    b, g = lax.axis_index("band"), lax.axis_index("grid")
    m, xh, xl, c = b // 2, b % 2, g // 2, g % 2
    far, near = (g + 2) % 4, g + 1 - 2 * c
    across, core, diagonal = at(b, far), at(b, near), at(b, 3 - g)
    up, up_far = at((b + 1) % 32, g), at((b + 1) % 32, far)
    down, down_far = at((b + 31) % 32, g), at((b + 31) % 32, far)
    low_m = (m + 15 + xh) % 16
    fetch = pltpu.make_async_copy(orb_hbm, orb, load_sem.at[0])
    fetch.start()
    fetch_table = pltpu.make_async_copy(h_hbm, h_ref, load_sem.at[1])
    fetch_table.start()
    barrier = pltpu.get_barrier_semaphore()
    for peer in (up, up_far, down, down_far, across, core, diagonal):
        pl.semaphore_signal(barrier, inc=1, device_id=peer, device_id_type=MESH)

    def greet(k, _):
        peer = at(2 * ((m + k) % 16) + xh, g)
        pl.semaphore_signal(barrier, inc=1, device_id=peer, device_id_type=MESH)
        return 0

    lax.fori_loop(1, 16, greet, 0)
    fetch.wait()
    for n in range(4):
        for t in range(18):
            ch, tile = divmod(t, TILES)
            own[n, pl.ds(ch * SPAN + tile, 12, stride=TILES), :] = orb[pl.ds(4 * t + n, 12, stride=72), :]
    for ch in range(CHUNKS):
        a_ref[:, part_rows(g, ch), :] = own[:, ch * SPAN : (ch + 1) * SPAN, :]
    pl.semaphore_wait(barrier, 22)

    def remote(sends, recvs, sem, recv_sem, src, dst, peer):
        return pltpu.make_async_remote_copy(
            src_ref=src, dst_ref=dst, send_sem=sends.at[sem], recv_sem=recvs.at[recv_sem],
            device_id=peer, device_id_type=MESH,
        )

    def first(kind, ch, src, dst, peer):
        return remote(gsend, grecv, kind, CHUNKS * kind + ch, src, dst, peer)

    def same(kind, ch, ref, owner, peer):
        where = ref.at[:, part_rows(owner, ch), :]
        return first(kind, ch, where, where, peer)

    def a_across(ch):
        return same(0, ch, a_ref, g, across)

    def b_wide(ch):
        src = a_ref.at[pl.ds(2 * xl, 2), part_rows(g, ch), :]
        return first(1, ch, src, b_ref.at[:, part_rows(g, ch), :], up)

    def b_near(ch):
        src = a_ref.at[pl.ds(2 - 2 * xl, 2), part_rows(g, ch), :]
        return first(2, ch, src, b_ref.at[:, part_rows(g, ch), :], up_far)

    def a_core(ch):
        return same(3, ch, a_ref, g, core)

    def a_far(ch):
        return same(4, ch, a_ref, far, core)

    def b_core(ch):
        return same(5, ch, b_ref, far, core)

    def b_far(ch):
        return same(6, ch, b_ref, g, core)

    def low_across(ch):
        target = low.at[pl.ds(2 * xl, 2), pl.ds(ch * SPAN, SPAN), :]
        return first(7, ch, b_ref.at[:, part_rows(far, ch), :], target, across)

    def low_in(ch):
        target = low.at[pl.ds(2 - 2 * xl, 2), pl.ds(ch * SPAN, SPAN), :]
        return first(7, ch, b_ref.at[:, part_rows(far, ch), :], target, across)

    a_whole, b_whole, b_half = a_ref.at[:, 0:SLAB, :], b_ref.at[:, 0:SLAB, :], a_ref.at[0:2, 0:SLAB, :]
    gathers = [first(kind, 0, w, w, across) for kind, w in enumerate((a_whole, b_half, b_half, a_whole, a_whole, b_whole, b_whole, b_whole))]

    def tile_rows(tile):
        return pl.ds(pl.multiple_of(8 * tile, 8), 8)

    def scatter(source, block, half, which, ch):
        def start(k, _):
            tile = 9 * ch + (k + m) % 9
            n, slot = tile % 16, tile // 16
            target = o_all.at[block, half, :, pl.ds(pl.multiple_of(8 * slot, 8), 8), :]
            copy = remote(osend, orecv, which, which, source.at[:, tile_rows(tile), :], target, at(2 * n + xh, g))
            pl.when(n != m)(copy.start)
            return 0

        lax.fori_loop(0, 9, start, 0)

    def keep_own(source, block, half):
        o_all[block, half, :, 0:8, :] = source[:, tile_rows(m), :]
        o_all[block, half, :, 8:16, :] = source[:, tile_rows(jnp.where(m <= 10, m + 16, m)), :]

    def scattered(which):
        def wait(sent, rows):
            window = own.at[:, 0 : 8 * sent, :]
            remote(osend, orecv, which, which, window, window, across).wait_send()
            window = o_all.at[0:15, 0, :, 0:rows, :]
            remote(osend, orecv, which, which, window, window, across).wait_recv()

        @pl.when(m <= 10)
        def _():
            wait(25, 16)

        @pl.when(m > 10)
        def _():
            wait(26, 8)

    def low_chunk(ch):
        with jax.named_scope("low"):
            low_in(ch).wait_recv()
            low[pl.ds(2 * xl, 2), pl.ds(ch * SPAN, SPAN), :] = b_ref[:, part_rows(g, ch), :]
            scatter(low, low_m, 1 - xh, 1, ch)

    d = 2 * c + xl

    def rows(ch, tile):
        return pl.ds(ch * 4 * SPAN + tile, NG, stride=TILES)

    def load(ref, i, ch, tile):
        return jnp.concatenate([ref[i, rows(ch, tile), :], ref[i, rows(ch, tile + 1), :]], axis=1)

    def store(ref, j, ch, tile, value):
        ref[j, rows(ch, tile), :] = value[:, :128]
        ref[j, rows(ch, tile + 1), :] = value[:, 128:]

    def forward(ch):
        for tile in range(0, TILES, 2):
            t = ch * TILES + tile
            single = load(a_ref, d, ch, tile)
            a0, a1 = load(a_ref, 2 * c, ch, tile), load(a_ref, 2 * c + 1, ch, tile)
            b0, b1 = load(b_ref, 0, ch, tile), load(b_ref, 1, ch, tile)
            for f in range(8):
                left = (a0, a0, a1, a1)[f] if f < 4 else single
                right = (b0, b1, b0, b1)[f] if f < 4 else load(a_ref, f - 4, ch, tile)
                out = hartley(table, left * right)
                s_ref[t, f * 48 : (f + 1) * 48, :] = out[:, :128]
                s_ref[t + 1, f * 48 : (f + 1) * 48, :] = out[:, 128:]

    def block_of(n, i):
        y, z = divmod(n * 8, 48)
        return pl.ds((i * 8 + y) * PITCH + z, 8)

    def turn_in(ch):
        def step(i, _):
            for v in range(3):
                for l in range(3):
                    block = s_ref[i * 3 + v, l * 128 : (l + 1) * 128, :].T
                    for n in range(16):
                        r_ref[l, block_of(v * 16 + n, i), :] = block[n * 8 : (n + 1) * 8, :]
            return 0

        lax.fori_loop(2 * ch, 2 * ch + 2, step, 0)

    def turn_out(ch):
        def step(i, _):
            for v in range(3):
                for l in range(3):
                    parts = [r_ref[l, block_of(v * 16 + n, i), :] for n in range(16)]
                    s_ref[i * 3 + v, l * 128 : (l + 1) * 128, :] = jnp.concatenate(parts, axis=0).T
            return 0

        lax.fori_loop(2 * ch, 2 * ch + 2, step, 0)

    def passes(source, target, where, count, scale=None):
        tiles = [(u, l) for u in range(count) for l in range(3)]
        for p in range(0, len(tiles), 2):
            pair = tiles[p : p + 2]
            value = jnp.concatenate([source[l, where(u), :] for u, l in pair], axis=1)
            out = hartley(table, value)
            for j, (u, l) in enumerate(pair):
                piece = out[:, 128 * j : 128 * (j + 1)]
                if scale is not None:
                    piece = piece * k_ref[l, scale(u), :]
                target[l, where(u), :] = piece

    def along_z(ch, source, target):
        passes(source, target, lambda u: pl.ds((16 * ch + u) * PITCH, 48), 16)

    def along_y(source, target, scaled):
        def step(i, _):
            passes(source, target, lambda u: pl.ds(i * U3 + u, 48, stride=PITCH), U3,
                   (lambda u: pl.ds(pl.multiple_of((i * U3 + u) * 48, 8), 48)) if scaled else None)
            return 0

        lax.fori_loop(0, 48 // U3, step, 0)

    with jax.named_scope("start"):
        for ch in range(CHUNKS):
            for copy_of in (b_wide, b_near, a_across, a_core):
                copy_of(ch).start()
        for ch in range(CHUNKS):
            scatter(own, m, xh, 0, ch)
        keep_own(own, m, xh)
        fill_kernel(k_ref)
        fetch_table.wait()
    table = h_ref[...]
    for ch in range(CHUNKS):
        with jax.named_scope("gather"):
            b_near(ch).wait_recv()
            b_core(ch).start()
            a_across(ch).wait_recv()
            a_far(ch).start()
            b_wide(ch).wait_recv()
            b_far(ch).start()
            if ch == CHUNKS - 1:
                for early in range(CHUNKS):
                    low_across(early).start()
            for copy_of in (a_core, b_core, a_far, b_far):
                copy_of(ch).wait_recv()
        with jax.named_scope("forward"):
            forward(ch)
        with jax.named_scope("turn_in"):
            turn_in(ch)
        with jax.named_scope("along_z"):
            along_z(ch, r_ref, q_ref)
    with jax.named_scope("along_y"):
        along_y(q_ref, r_ref, True)
    with jax.named_scope("along_y"):
        along_y(r_ref, q_ref, False)

    def potential(f, t):
        span = slice(f * 48, (f + 1) * 48)
        return hartley(table, jnp.concatenate([s_ref[t, span, :], s_ref[t + 1, span, :]], axis=1))

    def backward(ch):
        for tile in range(0, TILES, 2):
            t = ch * TILES + tile
            b0, b1 = load(b_ref, 0, ch, tile), load(b_ref, 1, ch, tile)
            a0, a1 = load(a_ref, 2 * c, ch, tile), load(a_ref, 2 * c + 1, ch, tile)
            p0, p1 = potential(0, t), potential(1, t)
            v0 = b0 * p0 + b1 * p1
            w0, w1 = a0 * p0, a0 * p1
            p2, p3 = potential(2, t), potential(3, t)
            v1 = b0 * p2 + b1 * p3
            store(ob, 0, ch, tile, -(w0 + a1 * p2))
            store(ob, 1, ch, tile, -(w1 + a1 * p3))
            extra = load(a_ref, 0, ch, tile) * potential(4, t)
            for j in range(1, 4):
                extra = extra + load(a_ref, j, ch, tile) * potential(4 + j, t)
            store(va, 0, ch, tile, -(v0 + jnp.where(xl == 0, extra, 0.0)))
            store(va, 1, ch, tile, -(v1 + jnp.where(xl == 0, 0.0, extra)))

    def second(kind, ch, src, dst, peer, recv_kind=None):
        recv_at = CHUNKS * (kind if recv_kind is None else recv_kind) + ch
        return remote(send, recv, kind, recv_at, src, dst, peer)

    def to_far(ch):
        return second(0, ch, va.at[:, part_rows(far, ch), :], back1.at[ch], across)

    def to_core(ch):
        return second(1, ch, va.at[:, part_rows(near, ch), :], back2.at[ch], core)

    def to_diagonal(ch):
        return second(2, ch, va.at[:, part_rows(3 - g, ch), :], back3.at[ch], diagonal)

    def owed_core(j, ch):
        return second(3 + j, ch, ob.at[:, part_rows(2 * j + 1 - c, ch), :], owed1.at[ch, j], core)

    def owed(j, ch):
        return second(5 + j, ch, sums.at[ch, j], owed3.at[ch, xl], at((b + 31) % 32, 2 * j + c), 5 + xl)

    def owed_in(j, ch):
        return second(5 + j, ch, sums.at[ch, j], owed3.at[ch, j], down)

    def hand_out(ch):
        owed_core(0, ch).start()
        owed_core(1, ch).start()
        if ch == 0:
            to_far(ch).start()
            to_diagonal(ch).start()
        to_core(ch).start()

    def pass_owed(ch):
        for j in range(2):
            owed_core(j, ch).wait_recv()
            sums[ch, j] = ob[:, part_rows(2 * j + c, ch), :] + owed1[ch, j]
            owed(j, ch).start()
        if ch > 0:
            to_far(ch).start()
            to_diagonal(ch).start()

    def spread(ch, j):
        tile = 9 * ch + j
        n, slot = tile % 16, tile // 16
        source = vec.at[:, :, tile_rows(tile), :]
        target = vc.at[m, :, :, pl.ds(pl.multiple_of(8 * slot, 8), 8), :]
        return remote(vsend, vrecv, 0, slot, source, target, at(2 * n + xh, g)), n

    def spread_sent(count):
        window = vec.at[:, :, pl.ds(0, 8 * count), :]
        remote(vsend, vrecv, 0, 0, window, window, across).wait_send()

    def spread_in(slot):
        window = vc.at[0:15, :, :, pl.ds(8 * slot, 8), :]
        remote(vsend, vrecv, 0, slot, window, window, across).wait_recv()

    def collect(ch):
        for copy_of in (to_far, to_core, to_diagonal):
            copy_of(ch).wait_recv()
        for j in range(2):
            owed_in(j, ch).wait_recv()
        where = pl.ds(ch * SPAN, SPAN)
        for e in range(2):
            vec[e, c, where, :] = va[e, part_rows(g, ch), :] + back1[ch, e] + owed3[ch, c, e]
            vec[e, 1 - c, where, :] = back2[ch, e] + back3[ch, e] + owed3[ch, 1 - c, e]

        def start(k, _):
            copy, n = spread(ch, (k + m) % 9)

            @pl.when(n != m)
            def _():
                copy.start()

            return 0

        lax.fori_loop(0, 9, start, 0)
        for t in range(TILES * ch, TILES * ch + TILES):
            place = pl.ds(ch * SPAN + t % TILES, 12, stride=TILES)
            for e in range(2):
                for n in range(2):
                    v_out[pl.ds(4 * t + 2 * n + e, 12, stride=72), :] = vec[e, n, place, :]

    for ch in range(CHUNKS):
        with jax.named_scope("along_z"):
            along_z(ch, q_ref, r_ref)
        if ch == 1:
            low_chunk(1)
        with jax.named_scope("turn_out"):
            turn_out(ch)
        if ch == 1:
            low_chunk(2)
            keep_own(low, low_m, 1 - xh)
        if ch > 0:
            with jax.named_scope("pass_owed"):
                pass_owed(ch - 1)
        with jax.named_scope("backward"):
            backward(ch)
            hand_out(ch)
        if ch == 0:
            low_chunk(0)
    with jax.named_scope("pass_owed"):
        pass_owed(CHUNKS - 1)
        for sent in gathers:
            sent.wait_send()
    for ch in range(CHUNKS):
        with jax.named_scope("collect"):
            collect(ch)
    with jax.named_scope("spread_wait"):
        vc[m, :, :, 0:8, :] = vec[:, :, tile_rows(m), :]
        vc[m, :, :, 8:16, :] = vec[:, :, tile_rows(jnp.where(m <= 10, m + 16, m)), :]
        for kind, w in enumerate((va, va, va, ob, ob, sums, sums)):
            if kind < 5:
                whole = w.at[:, 0:SLAB, :]
            else:
                whole = w.at[:, 0]
            remote(send, recv, kind, kind, whole, whole, across).wait_send()
        scattered(0)
        scattered(1)

        spread_in(0)

    dims = (((1,), (1,)), ((), ()))
    o_rows, v_rows = o_all.reshape(2048, 128), vc.reshape(1024, 128)

    def products(start):
        total = jnp.zeros((64, 128), F32)
        for r in range(start, start + 8):
            oh, ol = split(o_rows[pl.ds(r, 128, stride=16), :])
            vh, vl = split(v_rows[pl.ds(r, 64, stride=16), :])
            left = jnp.concatenate([vh, vl, vh], axis=1)
            right = jnp.concatenate([oh, oh, ol], axis=1)
            total = total + lax.dot_general(left, right, dims, preferred_element_type=F32)
        return total

    with jax.named_scope("products_first"):
        summed[...] = products(0)
    with jax.named_scope("spread_last"):

        @pl.when(m <= 10)
        def _():
            spread_in(1)
            summed[...] = summed[...] + products(8)
            spread_sent(25)

        @pl.when(m > 10)
        def _():
            spread_sent(26)

    with jax.named_scope("arrange"):
        total = summed[...]
        total = total * (1.0 / NCELL)
        lane = lax.broadcasted_iota(jnp.int32, (16, 128), 1) // 32
        slots = (0, 2, 1, 3)
        kinds = [jnp.concatenate([total[4 * n + k : 4 * n + k + 1] for n in range(16)], axis=0) for k in slots]
        for q in range(4):
            row = kinds[q]
            for k in range(4):
                if k != q:
                    row = jnp.where(lane == k, pltpu.roll(kinds[k], 32 * ((k - q) % 4), 1), row)
            for n in range(16):
                part[4 * n + q] = row[n : n + 1, :]

    def deal_start(k, _):
        n = (m + k) % 16
        for j in range(4):
            q = (g + j) % 4
            copy = remote(psend, precv, 0, 0, part.at[4 * n + q], rows_in.at[4 * k + j], at(2 * n + xh, q))
            if j > 0:
                copy.start()
            else:
                pl.when(k < 16)(copy.start)
        return 0

    with jax.named_scope("deal"):
        lax.fori_loop(1, 17, deal_start, 0)
        window = rows_in.at[4:67]
        remote(psend, precv, 0, 0, window, window, across).wait()
        whole = part[4 * m + g]
        for k in range(4, 68):
            if k != 64:
                whole = whole + rows_in[k]
        for k in range(4):
            m_out[k : k + 1, :] = whole[:, 32 * k : 32 * (k + 1)]


def on_device(orbitals):
    shape = jax.ShapeDtypeStruct
    dma = pltpu.SemaphoreType.DMA

    def room(*dims):
        return pltpu.VMEM(dims, F32)

    packed = orbitals.reshape(4, SLAB, 128).transpose(1, 0, 2).reshape(4 * SLAB, 128)
    triple = room(CHUNKS, 2, SPAN, 128)
    pairs = room(CHUNKS, 2, 2, SPAN, 128)
    vectors, margin = pl.pallas_call(
        exchange_kernel,
        out_shape=(pltpu.VMEM((4 * SLAB, 128), F32), pltpu.VMEM((4, 32), F32)),
        in_specs=[pl.BlockSpec(memory_space=pltpu.HBM)] * 2,
        out_specs=(VMEM, VMEM),
        scratch_shapes=[
            room(4 * SLAB, 128), pltpu.VMEM((NG, 3 * NG), BF16), dma((2,)), room(4, SLAB, 128), room(4, SLAB, 128),
            room(4, 864, 128), room(2, 864, 128), room(16, 2, 4, 16, 128), room(3, NG * NG, 128),
            room(18, 384, 128), room(3, NG * PITCH, 128), room(3, NG * PITCH, 128),
            room(2, 864, 128), room(2, 864, 128), pairs, pairs, pairs, triple, triple, triple,
            room(2, 2, SLAB, 128), room(16, 2, 2, 16, 128), room(64, 128),
            room(64, 1, 128), room(68, 1, 128),
            dma((8,)), dma((24,)), dma((2,)), dma((2,)), dma((7,)), dma((21,)),
            dma((1,)), dma((2,)), dma((1,)), dma((1,)),
        ],
        compiler_params=pltpu.CompilerParams(
            collective_id=0, has_side_effects=True, vmem_limit_bytes=56 * 1024 * 1024
        ),
        name="exchange",
    )(
        pltpu.with_memory_space_constraint(packed, pltpu.HBM),
        pltpu.with_memory_space_constraint(hartley_rows(), pltpu.HBM),
    )
    vectors = vectors.reshape(SLAB, 4, 128).transpose(1, 0, 2).reshape(4, SLAB * 128)
    return vectors, margin.T


def solution(mesh):
    return jax.shard_map(
        on_device,
        mesh=mesh,
        in_specs=(P("band", "grid"),),
        out_specs=(P("band", "grid"), P("grid", "band")),
        check_vma=False,
    )
```

```python
import jax
import jax.numpy as jnp
import numpy as np
from jax import lax
from jax.experimental import pallas as pl
from jax.experimental.pallas import tpu as pltpu
from jax.sharding import PartitionSpec as P

NG = 48
NCELL = 110592
PITCH = 52
SLAB = 216
MESH = pl.DeviceIdType.MESH
F32 = jnp.float32
BF16 = jnp.bfloat16
CHUNKS, TILES, SPAN = 3, 6, 72
U3 = 48
VMEM = pl.BlockSpec(memory_space=pltpu.VMEM)


def hartley_rows():
    index = np.arange(NG)
    angles = (index[:, None] * index[None, :] % NG) * (2 * np.pi / NG)
    table = (np.cos(angles) + np.sin(angles)).astype(np.float32)
    high = table.astype(BF16)
    low = (table - high.astype(np.float32)).astype(BF16)
    return jnp.asarray(np.concatenate([high, high, low], axis=1))


def folded(index):
    return ((index + NG // 2) % NG - NG // 2).astype(F32)


def at(b, g):
    return {"band": b, "grid": g}


def part_rows(g, ch):
    return pl.ds(pl.multiple_of(ch * 4 * SPAN + g * SPAN, 8), SPAN)


def split(value):
    high = value.astype(BF16)
    low = (value - high.astype(F32)).astype(BF16)
    return high, low


def hartley(table, value):
    high, low = split(value)
    stack = jnp.concatenate([high, low, high], axis=0)
    dims = (((1,), (0,)), ((), ()))
    return lax.dot_general(table, stack, dims, preferred_element_type=F32)


def fill_kernel(k_ref):
    lane = lax.broadcasted_iota(jnp.int32, (1, 128), 1)
    y = folded(lax.broadcasted_iota(jnp.int32, (NG, 128), 0))
    x = [folded((l * 128 + lane) % NG) for l in range(3)]
    planes = [y * y + v * v for v in x]

    def plane(z, _):
        depth = z.astype(F32)
        depth = depth * depth
        for l in range(3):
            square = planes[l] + depth
            safe = jnp.where(square > 0, square, 1.0)
            value = (40.0 / NCELL) * (1.0 - jnp.exp(-square / 16.0)) / safe
            value = jnp.where(square > 0, value, 0.0)
            k_ref[l, pl.ds(pl.multiple_of(z * NG, 8), NG), :] = value
        return 0

    lax.fori_loop(0, NG // 2 + 1, plane, 0)

    def mirror(z, _):
        for l in range(3):
            source = pl.ds(pl.multiple_of((NG - z) * NG, 8), NG)
            k_ref[l, pl.ds(pl.multiple_of(z * NG, 8), NG), :] = k_ref[l, source, :]
        return 0

    lax.fori_loop(NG // 2 + 1, NG, mirror, 0)


def exchange_kernel(orb_hbm, h_hbm, v_out, m_out, orb, h_ref, load_sem, own, low, a_ref, b_ref, o_all, k_ref, s_ref, r_ref, q_ref,
                    va, ob, owed1, sums, owed3, back1, back2, back3, vec, vc, summed, part, rows_in,
                    gsend, grecv, osend, orecv, send, recv, vsend, vrecv, psend, precv):
    b, g = lax.axis_index("band"), lax.axis_index("grid")
    m, xh, xl, c = b // 2, b % 2, g // 2, g % 2
    far, near = (g + 2) % 4, g + 1 - 2 * c
    across, core, diagonal = at(b, far), at(b, near), at(b, 3 - g)
    up, up_far = at((b + 1) % 32, g), at((b + 1) % 32, far)
    down, down_far = at((b + 31) % 32, g), at((b + 31) % 32, far)
    low_m = (m + 15 + xh) % 16
    fetch = pltpu.make_async_copy(orb_hbm, orb, load_sem.at[0])
    fetch.start()
    fetch_table = pltpu.make_async_copy(h_hbm, h_ref, load_sem.at[1])
    fetch_table.start()
    barrier = pltpu.get_barrier_semaphore()
    for peer in (up, up_far, down, down_far, across, core, diagonal):
        pl.semaphore_signal(barrier, inc=1, device_id=peer, device_id_type=MESH)

    def greet(k, _):
        peer = at(2 * ((m + k) % 16) + xh, g)
        pl.semaphore_signal(barrier, inc=1, device_id=peer, device_id_type=MESH)
        return 0

    lax.fori_loop(1, 16, greet, 0)
    fetch.wait()
    for n in range(4):
        for t in range(18):
            ch, tile = divmod(t, TILES)
            own[n, pl.ds(ch * SPAN + tile, 12, stride=TILES), :] = orb[pl.ds(4 * t + n, 12, stride=72), :]
    for ch in range(CHUNKS):
        a_ref[:, part_rows(g, ch), :] = own[:, ch * SPAN : (ch + 1) * SPAN, :]
    pl.semaphore_wait(barrier, 22)

    def remote(sends, recvs, sem, recv_sem, src, dst, peer):
        return pltpu.make_async_remote_copy(
            src_ref=src, dst_ref=dst, send_sem=sends.at[sem], recv_sem=recvs.at[recv_sem],
            device_id=peer, device_id_type=MESH,
        )

    def first(kind, ch, src, dst, peer):
        return remote(gsend, grecv, kind, CHUNKS * kind + ch, src, dst, peer)

    def same(kind, ch, ref, owner, peer):
        where = ref.at[:, part_rows(owner, ch), :]
        return first(kind, ch, where, where, peer)

    def a_across(ch):
        return same(0, ch, a_ref, g, across)

    def b_wide(ch):
        src = a_ref.at[pl.ds(2 * xl, 2), part_rows(g, ch), :]
        return first(1, ch, src, b_ref.at[:, part_rows(g, ch), :], up)

    def b_near(ch):
        src = a_ref.at[pl.ds(2 - 2 * xl, 2), part_rows(g, ch), :]
        return first(2, ch, src, b_ref.at[:, part_rows(g, ch), :], up_far)

    def a_core(ch):
        return same(3, ch, a_ref, g, core)

    def a_far(ch):
        return same(4, ch, a_ref, far, core)

    def b_core(ch):
        return same(5, ch, b_ref, far, core)

    def b_far(ch):
        return same(6, ch, b_ref, g, core)

    def low_across(ch):
        target = low.at[pl.ds(2 * xl, 2), pl.ds(ch * SPAN, SPAN), :]
        return first(7, ch, b_ref.at[:, part_rows(far, ch), :], target, across)

    def low_in(ch):
        target = low.at[pl.ds(2 - 2 * xl, 2), pl.ds(ch * SPAN, SPAN), :]
        return first(7, ch, b_ref.at[:, part_rows(far, ch), :], target, across)

    a_whole, b_whole, b_half = a_ref.at[:, 0:SLAB, :], b_ref.at[:, 0:SLAB, :], a_ref.at[0:2, 0:SLAB, :]
    gathers = [first(kind, 0, w, w, across) for kind, w in enumerate((a_whole, b_half, b_half, a_whole, a_whole, b_whole, b_whole, b_whole))]

    def tile_rows(tile):
        return pl.ds(pl.multiple_of(8 * tile, 8), 8)

    def scatter(source, block, half, which, ch):
        def start(k, _):
            tile = 9 * ch + (k + m) % 9
            n, slot = tile % 16, tile // 16
            target = o_all.at[block, half, :, pl.ds(pl.multiple_of(8 * slot, 8), 8), :]
            copy = remote(osend, orecv, which, which, source.at[:, tile_rows(tile), :], target, at(2 * n + xh, g))
            pl.when(n != m)(copy.start)
            return 0

        lax.fori_loop(0, 9, start, 0)

    def keep_own(source, block, half):
        o_all[block, half, :, 0:8, :] = source[:, tile_rows(m), :]
        o_all[block, half, :, 8:16, :] = source[:, tile_rows(jnp.where(m <= 10, m + 16, m)), :]

    def scattered(which):
        def wait(sent, rows):
            window = own.at[:, 0 : 8 * sent, :]
            remote(osend, orecv, which, which, window, window, across).wait_send()
            window = o_all.at[0:15, 0, :, 0:rows, :]
            remote(osend, orecv, which, which, window, window, across).wait_recv()

        @pl.when(m <= 10)
        def _():
            wait(25, 16)

        @pl.when(m > 10)
        def _():
            wait(26, 8)

    def low_chunk(ch):
        with jax.named_scope("low"):
            low_in(ch).wait_recv()
            low[pl.ds(2 * xl, 2), pl.ds(ch * SPAN, SPAN), :] = b_ref[:, part_rows(g, ch), :]
            scatter(low, low_m, 1 - xh, 1, ch)

    d = 2 * c + xl

    def rows(ch, tile):
        return pl.ds(ch * 4 * SPAN + tile, NG, stride=TILES)

    def load(ref, i, ch, tile):
        return jnp.concatenate([ref[i, rows(ch, tile), :], ref[i, rows(ch, tile + 1), :]], axis=1)

    def store(ref, j, ch, tile, value):
        ref[j, rows(ch, tile), :] = value[:, :128]
        ref[j, rows(ch, tile + 1), :] = value[:, 128:]

    def forward(ch):
        for tile in range(0, TILES, 2):
            t = ch * TILES + tile
            single = load(a_ref, d, ch, tile)
            a0, a1 = load(a_ref, 2 * c, ch, tile), load(a_ref, 2 * c + 1, ch, tile)
            b0, b1 = load(b_ref, 0, ch, tile), load(b_ref, 1, ch, tile)
            for f in range(8):
                left = (a0, a0, a1, a1)[f] if f < 4 else single
                right = (b0, b1, b0, b1)[f] if f < 4 else load(a_ref, f - 4, ch, tile)
                out = hartley(table, left * right)
                s_ref[t, f * 48 : (f + 1) * 48, :] = out[:, :128]
                s_ref[t + 1, f * 48 : (f + 1) * 48, :] = out[:, 128:]

    def block_of(n, i):
        y, z = divmod(n * 8, 48)
        return pl.ds((i * 8 + y) * PITCH + z, 8)

    def turn_in(ch):
        def step(i, _):
            for v in range(3):
                for l in range(3):
                    block = s_ref[i * 3 + v, l * 128 : (l + 1) * 128, :].T
                    for n in range(16):
                        r_ref[l, block_of(v * 16 + n, i), :] = block[n * 8 : (n + 1) * 8, :]
            return 0

        for i in (2 * ch, 2 * ch + 1):
            step(i, 0)

    def turn_out(ch):
        def step(i, _):
            for v in range(3):
                for l in range(3):
                    parts = [r_ref[l, block_of(v * 16 + n, i), :] for n in range(16)]
                    s_ref[i * 3 + v, l * 128 : (l + 1) * 128, :] = jnp.concatenate(parts, axis=0).T
            return 0

        for i in (2 * ch, 2 * ch + 1):
            step(i, 0)

    def passes(source, target, where, count, scale=None):
        tiles = [(u, l) for u in range(count) for l in range(3)]
        for p in range(0, len(tiles), 2):
            pair = tiles[p : p + 2]
            value = jnp.concatenate([source[l, where(u), :] for u, l in pair], axis=1)
            out = hartley(table, value)
            for j, (u, l) in enumerate(pair):
                piece = out[:, 128 * j : 128 * (j + 1)]
                if scale is not None:
                    piece = piece * k_ref[l, scale(u), :]
                target[l, where(u), :] = piece

    def along_z(ch, source, target):
        passes(source, target, lambda u: pl.ds((16 * ch + u) * PITCH, 48), 16)

    def along_y(source, target, scaled):
        def step(i, _):
            passes(source, target, lambda u: pl.ds(i * U3 + u, 48, stride=PITCH), U3,
                   (lambda u: pl.ds(pl.multiple_of((i * U3 + u) * 48, 8), 48)) if scaled else None)
            return 0

        lax.fori_loop(0, 48 // U3, step, 0)

    with jax.named_scope("start"):
        for ch in range(CHUNKS):
            for copy_of in (b_wide, b_near, a_across, a_core):
                copy_of(ch).start()
        for ch in range(CHUNKS):
            scatter(own, m, xh, 0, ch)
        keep_own(own, m, xh)
        fill_kernel(k_ref)
        fetch_table.wait()
    table = h_ref[...]
    for ch in range(CHUNKS):
        with jax.named_scope("gather"):
            b_near(ch).wait_recv()
            b_core(ch).start()
            a_across(ch).wait_recv()
            a_far(ch).start()
            b_wide(ch).wait_recv()
            b_far(ch).start()
            if ch == CHUNKS - 1:
                for early in range(CHUNKS):
                    low_across(early).start()
            for copy_of in (a_core, b_core, a_far, b_far):
                copy_of(ch).wait_recv()
        with jax.named_scope("forward"):
            forward(ch)
        with jax.named_scope("turn_in"):
            turn_in(ch)
        with jax.named_scope("along_z"):
            along_z(ch, r_ref, q_ref)
    with jax.named_scope("along_y"):
        along_y(q_ref, r_ref, True)
    with jax.named_scope("along_y"):
        along_y(r_ref, q_ref, False)

    def potential(f, t):
        span = slice(f * 48, (f + 1) * 48)
        return hartley(table, jnp.concatenate([s_ref[t, span, :], s_ref[t + 1, span, :]], axis=1))

    def backward(ch):
        for tile in range(0, TILES, 2):
            t = ch * TILES + tile
            b0, b1 = load(b_ref, 0, ch, tile), load(b_ref, 1, ch, tile)
            a0, a1 = load(a_ref, 2 * c, ch, tile), load(a_ref, 2 * c + 1, ch, tile)
            p0, p1 = potential(0, t), potential(1, t)
            v0 = b0 * p0 + b1 * p1
            w0, w1 = a0 * p0, a0 * p1
            p2, p3 = potential(2, t), potential(3, t)
            v1 = b0 * p2 + b1 * p3
            store(ob, 0, ch, tile, -(w0 + a1 * p2))
            store(ob, 1, ch, tile, -(w1 + a1 * p3))
            extra = load(a_ref, 0, ch, tile) * potential(4, t)
            for j in range(1, 4):
                extra = extra + load(a_ref, j, ch, tile) * potential(4 + j, t)
            store(va, 0, ch, tile, -(v0 + jnp.where(xl == 0, extra, 0.0)))
            store(va, 1, ch, tile, -(v1 + jnp.where(xl == 0, 0.0, extra)))

    def second(kind, ch, src, dst, peer, recv_kind=None):
        recv_at = CHUNKS * (kind if recv_kind is None else recv_kind) + ch
        return remote(send, recv, kind, recv_at, src, dst, peer)

    def to_far(ch):
        return second(0, ch, va.at[:, part_rows(far, ch), :], back1.at[ch], across)

    def to_core(ch):
        return second(1, ch, va.at[:, part_rows(near, ch), :], back2.at[ch], core)

    def to_diagonal(ch):
        return second(2, ch, va.at[:, part_rows(3 - g, ch), :], back3.at[ch], diagonal)

    def owed_core(j, ch):
        return second(3 + j, ch, ob.at[:, part_rows(2 * j + 1 - c, ch), :], owed1.at[ch, j], core)

    def owed(j, ch):
        return second(5 + j, ch, sums.at[ch, j], owed3.at[ch, xl], at((b + 31) % 32, 2 * j + c), 5 + xl)

    def owed_in(j, ch):
        return second(5 + j, ch, sums.at[ch, j], owed3.at[ch, j], down)

    def hand_out(ch):
        owed_core(0, ch).start()
        owed_core(1, ch).start()
        if ch == 0:
            to_far(ch).start()
            to_diagonal(ch).start()
        to_core(ch).start()

    def pass_owed(ch):
        for j in range(2):
            owed_core(j, ch).wait_recv()
            sums[ch, j] = ob[:, part_rows(2 * j + c, ch), :] + owed1[ch, j]
            owed(j, ch).start()
        if ch > 0:
            to_far(ch).start()
            to_diagonal(ch).start()

    def spread(ch, j):
        tile = 9 * ch + j
        n, slot = tile % 16, tile // 16
        source = vec.at[:, :, tile_rows(tile), :]
        target = vc.at[m, :, :, pl.ds(pl.multiple_of(8 * slot, 8), 8), :]
        return remote(vsend, vrecv, 0, slot, source, target, at(2 * n + xh, g)), n

    def spread_sent(count):
        window = vec.at[:, :, pl.ds(0, 8 * count), :]
        remote(vsend, vrecv, 0, 0, window, window, across).wait_send()

    def spread_in(slot):
        window = vc.at[0:15, :, :, pl.ds(8 * slot, 8), :]
        remote(vsend, vrecv, 0, slot, window, window, across).wait_recv()

    def collect(ch):
        for copy_of in (to_far, to_core, to_diagonal):
            copy_of(ch).wait_recv()
        for j in range(2):
            owed_in(j, ch).wait_recv()
        where = pl.ds(ch * SPAN, SPAN)
        for e in range(2):
            vec[e, c, where, :] = va[e, part_rows(g, ch), :] + back1[ch, e] + owed3[ch, c, e]
            vec[e, 1 - c, where, :] = back2[ch, e] + back3[ch, e] + owed3[ch, 1 - c, e]

        def start(k, _):
            copy, n = spread(ch, (k + m) % 9)

            @pl.when(n != m)
            def _():
                copy.start()

            return 0

        lax.fori_loop(0, 9, start, 0)
        for t in range(TILES * ch, TILES * ch + TILES):
            place = pl.ds(ch * SPAN + t % TILES, 12, stride=TILES)
            for e in range(2):
                for n in range(2):
                    v_out[pl.ds(4 * t + 2 * n + e, 12, stride=72), :] = vec[e, n, place, :]

    for ch in range(CHUNKS):
        with jax.named_scope("along_z"):
            along_z(ch, q_ref, r_ref)
        if ch > 0:
            with jax.named_scope("pass_owed"):
                pass_owed(ch - 1)
        with jax.named_scope("turn_out"):
            turn_out(ch)
        if ch > 0:
            low_chunk(ch - 1)
        with jax.named_scope("backward"):
            backward(ch)
            hand_out(ch)
    with jax.named_scope("pass_owed"):
        pass_owed(CHUNKS - 1)
        low_chunk(CHUNKS - 1)
        keep_own(low, low_m, 1 - xh)
        for sent in gathers:
            sent.wait_send()
    for ch in range(CHUNKS):
        with jax.named_scope("collect"):
            collect(ch)
    with jax.named_scope("spread_wait"):
        vc[m, :, :, 0:8, :] = vec[:, :, tile_rows(m), :]
        vc[m, :, :, 8:16, :] = vec[:, :, tile_rows(jnp.where(m <= 10, m + 16, m)), :]
        for kind, w in enumerate((va, va, va, ob, ob, sums, sums)):
            if kind < 5:
                whole = w.at[:, 0:SLAB, :]
            else:
                whole = w.at[:, 0]
            remote(send, recv, kind, kind, whole, whole, across).wait_send()
        scattered(0)
        scattered(1)

        spread_in(0)

    dims = (((1,), (1,)), ((), ()))
    o_rows, v_rows = o_all.reshape(2048, 128), vc.reshape(1024, 128)

    def products(start):
        total = jnp.zeros((64, 128), F32)
        for r in range(start, start + 8):
            oh, ol = split(o_rows[pl.ds(r, 128, stride=16), :])
            vh, vl = split(v_rows[pl.ds(r, 64, stride=16), :])
            left = jnp.concatenate([vh, vl, vh], axis=1)
            right = jnp.concatenate([oh, oh, ol], axis=1)
            total = total + lax.dot_general(left, right, dims, preferred_element_type=F32)
        return total

    with jax.named_scope("products_first"):
        summed[...] = products(0)
    with jax.named_scope("spread_last"):

        @pl.when(m <= 10)
        def _():
            spread_in(1)
            summed[...] = summed[...] + products(8)
            spread_sent(25)

        @pl.when(m > 10)
        def _():
            spread_sent(26)

    with jax.named_scope("arrange"):
        total = summed[...]
        total = total * (1.0 / NCELL)
        lane = lax.broadcasted_iota(jnp.int32, (16, 128), 1) // 32
        slots = (0, 2, 1, 3)
        kinds = [jnp.concatenate([total[4 * n + k : 4 * n + k + 1] for n in range(16)], axis=0) for k in slots]
        for q in range(4):
            row = kinds[q]
            for k in range(4):
                if k != q:
                    row = jnp.where(lane == k, pltpu.roll(kinds[k], 32 * ((k - q) % 4), 1), row)
            for n in range(16):
                part[4 * n + q] = row[n : n + 1, :]

    def deal_start(k, _):
        n = (m + k) % 16
        for j in range(4):
            q = (g + j) % 4
            copy = remote(psend, precv, 0, 0, part.at[4 * n + q], rows_in.at[4 * k + j], at(2 * n + xh, q))
            if j > 0:
                copy.start()
            else:
                pl.when(k < 16)(copy.start)
        return 0

    with jax.named_scope("deal"):
        lax.fori_loop(1, 17, deal_start, 0)
        window = rows_in.at[4:67]
        remote(psend, precv, 0, 0, window, window, across).wait()
        whole = part[4 * m + g]
        for k in range(4, 68):
            if k != 64:
                whole = whole + rows_in[k]
        for k in range(4):
            m_out[k : k + 1, :] = whole[:, 32 * k : 32 * (k + 1)]


def on_device(orbitals):
    shape = jax.ShapeDtypeStruct
    dma = pltpu.SemaphoreType.DMA

    def room(*dims):
        return pltpu.VMEM(dims, F32)

    packed = orbitals.reshape(4, SLAB, 128).transpose(1, 0, 2).reshape(4 * SLAB, 128)
    triple = room(CHUNKS, 2, SPAN, 128)
    pairs = room(CHUNKS, 2, 2, SPAN, 128)
    vectors, margin = pl.pallas_call(
        exchange_kernel,
        out_shape=(pltpu.VMEM((4 * SLAB, 128), F32), pltpu.VMEM((4, 32), F32)),
        in_specs=[pl.BlockSpec(memory_space=pltpu.HBM)] * 2,
        out_specs=(VMEM, VMEM),
        scratch_shapes=[
            room(4 * SLAB, 128), pltpu.VMEM((NG, 3 * NG), BF16), dma((2,)), room(4, SLAB, 128), room(4, SLAB, 128),
            room(4, 864, 128), room(2, 864, 128), room(16, 2, 4, 16, 128), room(3, NG * NG, 128),
            room(18, 384, 128), room(3, NG * PITCH, 128), room(3, NG * PITCH, 128),
            room(2, 864, 128), room(2, 864, 128), pairs, pairs, pairs, triple, triple, triple,
            room(2, 2, SLAB, 128), room(16, 2, 2, 16, 128), room(64, 128),
            room(64, 1, 128), room(68, 1, 128),
            dma((8,)), dma((24,)), dma((2,)), dma((2,)), dma((7,)), dma((21,)),
            dma((1,)), dma((2,)), dma((1,)), dma((1,)),
        ],
        compiler_params=pltpu.CompilerParams(
            collective_id=0, has_side_effects=True, vmem_limit_bytes=56 * 1024 * 1024
        ),
        name="exchange",
    )(
        pltpu.with_memory_space_constraint(packed, pltpu.HBM),
        pltpu.with_memory_space_constraint(hartley_rows(), pltpu.HBM),
    )
    vectors = vectors.reshape(SLAB, 4, 128).transpose(1, 0, 2).reshape(4, SLAB * 128)
    return vectors, margin.T


def solution(mesh):
    return jax.shard_map(
        on_device,
        mesh=mesh,
        in_specs=(P("band", "grid"),),
        out_specs=(P("band", "grid"), P("grid", "band")),
        check_vma=False,
    )
```

```python
import jax
import jax.numpy as jnp
import numpy as np
from jax import lax
from jax.experimental import pallas as pl
from jax.experimental.pallas import tpu as pltpu
from jax.sharding import PartitionSpec as P

NG = 48
NCELL = 110592
PITCH = 52
SLAB = 216
MESH = pl.DeviceIdType.MESH
F32 = jnp.float32
BF16 = jnp.bfloat16
CHUNKS, TILES, SPAN = 3, 6, 72
U3 = 48
VMEM = pl.BlockSpec(memory_space=pltpu.VMEM)


def hartley_rows():
    index = np.arange(NG)
    angles = (index[:, None] * index[None, :] % NG) * (2 * np.pi / NG)
    table = (np.cos(angles) + np.sin(angles)).astype(np.float32)
    high = table.astype(BF16)
    low = (table - high.astype(np.float32)).astype(BF16)
    return jnp.asarray(np.concatenate([high, high, low], axis=1))


def folded(index):
    return ((index + NG // 2) % NG - NG // 2).astype(F32)


def at(b, g):
    return {"band": b, "grid": g}


def part_rows(g, ch):
    return pl.ds(pl.multiple_of(ch * 4 * SPAN + g * SPAN, 8), SPAN)


def split(value):
    high = value.astype(BF16)
    low = (value - high.astype(F32)).astype(BF16)
    return high, low


def hartley(table, value):
    high, low = split(value)
    stack = jnp.concatenate([high, low, high], axis=0)
    dims = (((1,), (0,)), ((), ()))
    return lax.dot_general(table, stack, dims, preferred_element_type=F32)


def fill_kernel(k_ref):
    lane = lax.broadcasted_iota(jnp.int32, (1, 128), 1)
    y = folded(lax.broadcasted_iota(jnp.int32, (NG, 128), 0))
    x = [folded((l * 128 + lane) % NG) for l in range(3)]
    planes = [y * y + v * v for v in x]

    def plane(z, _):
        depth = z.astype(F32)
        depth = depth * depth
        for l in range(3):
            square = planes[l] + depth
            safe = jnp.where(square > 0, square, 1.0)
            value = (40.0 / NCELL) * (1.0 - jnp.exp(-square / 16.0)) / safe
            value = jnp.where(square > 0, value, 0.0)
            k_ref[l, pl.ds(pl.multiple_of(z * NG, 8), NG), :] = value
        return 0

    lax.fori_loop(0, NG // 2 + 1, plane, 0)

    def mirror(z, _):
        for l in range(3):
            source = pl.ds(pl.multiple_of((NG - z) * NG, 8), NG)
            k_ref[l, pl.ds(pl.multiple_of(z * NG, 8), NG), :] = k_ref[l, source, :]
        return 0

    lax.fori_loop(NG // 2 + 1, NG, mirror, 0)


def exchange_kernel(orb_hbm, h_hbm, v_out, m_out, orb, h_ref, load_sem, own, low, a_ref, b_ref, o_all, k_ref, s_ref, r_ref, q_ref,
                    va, ob, owed1, sums, owed3, back1, back2, back3, vec, vc, summed, part, rows_in,
                    gsend, grecv, osend, orecv, send, recv, vsend, vrecv, psend, precv):
    b, g = lax.axis_index("band"), lax.axis_index("grid")
    m, xh, xl, c = b // 2, b % 2, g // 2, g % 2
    far, near = (g + 2) % 4, g + 1 - 2 * c
    across, core, diagonal = at(b, far), at(b, near), at(b, 3 - g)
    up, up_far = at((b + 1) % 32, g), at((b + 1) % 32, far)
    down, down_far = at((b + 31) % 32, g), at((b + 31) % 32, far)
    low_m = (m + 15 + xh) % 16
    fetch = pltpu.make_async_copy(orb_hbm, orb, load_sem.at[0])
    fetch.start()
    fetch_table = pltpu.make_async_copy(h_hbm, h_ref, load_sem.at[1])
    fetch_table.start()
    barrier = pltpu.get_barrier_semaphore()
    for peer in (up, up_far, down, down_far, across, core, diagonal):
        pl.semaphore_signal(barrier, inc=1, device_id=peer, device_id_type=MESH)

    def greet(k, _):
        peer = at(2 * ((m + k) % 16) + xh, g)
        pl.semaphore_signal(barrier, inc=1, device_id=peer, device_id_type=MESH)
        return 0

    lax.fori_loop(1, 16, greet, 0)
    fetch.wait()
    for n in range(4):
        for t in range(18):
            ch, tile = divmod(t, TILES)
            own[n, pl.ds(ch * SPAN + tile, 12, stride=TILES), :] = orb[pl.ds(4 * t + n, 12, stride=72), :]
    for ch in range(CHUNKS):
        a_ref[:, part_rows(g, ch), :] = own[:, ch * SPAN : (ch + 1) * SPAN, :]
    pl.semaphore_wait(barrier, 22)

    def remote(sends, recvs, sem, recv_sem, src, dst, peer):
        return pltpu.make_async_remote_copy(
            src_ref=src, dst_ref=dst, send_sem=sends.at[sem], recv_sem=recvs.at[recv_sem],
            device_id=peer, device_id_type=MESH,
        )

    def first(kind, ch, src, dst, peer):
        return remote(gsend, grecv, kind, CHUNKS * kind + ch, src, dst, peer)

    def same(kind, ch, ref, owner, peer):
        where = ref.at[:, part_rows(owner, ch), :]
        return first(kind, ch, where, where, peer)

    def a_across(ch):
        return same(0, ch, a_ref, g, across)

    def b_wide(ch):
        src = a_ref.at[pl.ds(2 * xl, 2), part_rows(g, ch), :]
        return first(1, ch, src, b_ref.at[:, part_rows(g, ch), :], up)

    def b_near(ch):
        src = a_ref.at[pl.ds(2 - 2 * xl, 2), part_rows(g, ch), :]
        return first(2, ch, src, b_ref.at[:, part_rows(g, ch), :], up_far)

    def a_core(ch):
        return same(3, ch, a_ref, g, core)

    def a_far(ch):
        return same(4, ch, a_ref, far, core)

    def b_core(ch):
        return same(5, ch, b_ref, far, core)

    def b_far(ch):
        return same(6, ch, b_ref, g, core)

    def low_across(ch):
        target = low.at[pl.ds(2 * xl, 2), pl.ds(ch * SPAN, SPAN), :]
        return first(7, ch, b_ref.at[:, part_rows(far, ch), :], target, across)

    def low_in(ch):
        target = low.at[pl.ds(2 - 2 * xl, 2), pl.ds(ch * SPAN, SPAN), :]
        return first(7, ch, b_ref.at[:, part_rows(far, ch), :], target, across)

    a_whole, b_whole, b_half = a_ref.at[:, 0:SLAB, :], b_ref.at[:, 0:SLAB, :], a_ref.at[0:2, 0:SLAB, :]
    gathers = [first(kind, 0, w, w, across) for kind, w in enumerate((a_whole, b_half, b_half, a_whole, a_whole, b_whole, b_whole, b_whole))]

    def tile_rows(tile):
        return pl.ds(pl.multiple_of(8 * tile, 8), 8)

    def scatter(source, block, half, which, ch):
        def start(k, _):
            tile = 9 * ch + (k + m) % 9
            n, slot = tile % 16, tile // 16
            target = o_all.at[block, half, :, pl.ds(pl.multiple_of(8 * slot, 8), 8), :]
            copy = remote(osend, orecv, which, which, source.at[:, tile_rows(tile), :], target, at(2 * n + xh, g))
            pl.when(n != m)(copy.start)
            return 0

        lax.fori_loop(0, 9, start, 0)

    def keep_own(source, block, half):
        o_all[block, half, :, 0:8, :] = source[:, tile_rows(m), :]
        o_all[block, half, :, 8:16, :] = source[:, tile_rows(jnp.where(m <= 10, m + 16, m)), :]

    def scattered(which):
        def wait(sent, rows):
            window = own.at[:, 0 : 8 * sent, :]
            remote(osend, orecv, which, which, window, window, across).wait_send()
            window = o_all.at[0:15, 0, :, 0:rows, :]
            remote(osend, orecv, which, which, window, window, across).wait_recv()

        @pl.when(m <= 10)
        def _():
            wait(25, 16)

        @pl.when(m > 10)
        def _():
            wait(26, 8)

    def low_chunk(ch):
        with jax.named_scope("low"):
            low_in(ch).wait_recv()
            low[pl.ds(2 * xl, 2), pl.ds(ch * SPAN, SPAN), :] = b_ref[:, part_rows(g, ch), :]
            scatter(low, low_m, 1 - xh, 1, ch)

    d = 2 * c + xl

    def rows(ch, tile):
        return pl.ds(ch * 4 * SPAN + tile, NG, stride=TILES)

    def load(ref, i, ch, tile):
        return jnp.concatenate([ref[i, rows(ch, tile), :], ref[i, rows(ch, tile + 1), :]], axis=1)

    def store(ref, j, ch, tile, value):
        ref[j, rows(ch, tile), :] = value[:, :128]
        ref[j, rows(ch, tile + 1), :] = value[:, 128:]

    def forward(ch):
        for tile in range(0, TILES, 2):
            t = ch * TILES + tile
            single = load(a_ref, d, ch, tile)
            a0, a1 = load(a_ref, 2 * c, ch, tile), load(a_ref, 2 * c + 1, ch, tile)
            b0, b1 = load(b_ref, 0, ch, tile), load(b_ref, 1, ch, tile)
            for f in range(8):
                left = (a0, a0, a1, a1)[f] if f < 4 else single
                right = (b0, b1, b0, b1)[f] if f < 4 else load(a_ref, f - 4, ch, tile)
                out = hartley(table, left * right)
                s_ref[t, f * 48 : (f + 1) * 48, :] = out[:, :128]
                s_ref[t + 1, f * 48 : (f + 1) * 48, :] = out[:, 128:]

    def block_of(n, i):
        y, z = divmod(n * 8, 48)
        return pl.ds((i * 8 + y) * PITCH + z, 8)

    def turn_in(ch):
        def step(i, _):
            for v in range(3):
                for l in range(3):
                    block = s_ref[i * 3 + v, l * 128 : (l + 1) * 128, :].T
                    for n in range(16):
                        r_ref[l, block_of(v * 16 + n, i), :] = block[n * 8 : (n + 1) * 8, :]
            return 0

        for i in (2 * ch, 2 * ch + 1):
            step(i, 0)

    def turn_out(ch):
        def step(i, _):
            for v in range(3):
                for l in range(3):
                    parts = [r_ref[l, block_of(v * 16 + n, i), :] for n in range(16)]
                    s_ref[i * 3 + v, l * 128 : (l + 1) * 128, :] = jnp.concatenate(parts, axis=0).T
            return 0

        for i in (2 * ch, 2 * ch + 1):
            step(i, 0)

    def passes(source, target, where, count, scale=None):
        tiles = [(u, l) for u in range(count) for l in range(3)]
        for p in range(0, len(tiles), 2):
            pair = tiles[p : p + 2]
            value = jnp.concatenate([source[l, where(u), :] for u, l in pair], axis=1)
            out = hartley(table, value)
            for j, (u, l) in enumerate(pair):
                piece = out[:, 128 * j : 128 * (j + 1)]
                if scale is not None:
                    piece = piece * k_ref[l, scale(u), :]
                target[l, where(u), :] = piece

    def along_z(ch, source, target):
        passes(source, target, lambda u: pl.ds((16 * ch + u) * PITCH, 48), 16)

    def along_y(source, target, scaled):
        def step(i, _):
            passes(source, target, lambda u: pl.ds(i * U3 + u, 48, stride=PITCH), U3,
                   (lambda u: pl.ds(pl.multiple_of((i * U3 + u) * 48, 8), 48)) if scaled else None)
            return 0

        lax.fori_loop(0, 48 // U3, step, 0)

    with jax.named_scope("start"):
        for ch in range(CHUNKS):
            for copy_of in (b_wide, b_near, a_across, a_core):
                copy_of(ch).start()
        for ch in range(CHUNKS):
            scatter(own, m, xh, 0, ch)
        keep_own(own, m, xh)
        fill_kernel(k_ref)
        fetch_table.wait()
    table = h_ref[...]
    for ch in range(CHUNKS):
        with jax.named_scope("gather"):
            b_near(ch).wait_recv()
            b_core(ch).start()
            b_wide(ch).wait_recv()
            b_far(ch).start()
            a_across(ch).wait_recv()
            a_far(ch).start()
            if ch == CHUNKS - 1:
                for early in range(CHUNKS):
                    low_across(early).start()
            for copy_of in (a_core, b_core, a_far, b_far):
                copy_of(ch).wait_recv()
        with jax.named_scope("forward"):
            forward(ch)
        with jax.named_scope("turn_in"):
            turn_in(ch)
        with jax.named_scope("along_z"):
            along_z(ch, r_ref, q_ref)
    with jax.named_scope("along_y"):
        along_y(q_ref, r_ref, True)
    with jax.named_scope("along_y"):
        along_y(r_ref, q_ref, False)

    def potential(f, t):
        span = slice(f * 48, (f + 1) * 48)
        return hartley(table, jnp.concatenate([s_ref[t, span, :], s_ref[t + 1, span, :]], axis=1))

    def backward(ch):
        for tile in range(0, TILES, 2):
            t = ch * TILES + tile
            b0, b1 = load(b_ref, 0, ch, tile), load(b_ref, 1, ch, tile)
            a0, a1 = load(a_ref, 2 * c, ch, tile), load(a_ref, 2 * c + 1, ch, tile)
            p0, p1 = potential(0, t), potential(1, t)
            v0 = b0 * p0 + b1 * p1
            w0, w1 = a0 * p0, a0 * p1
            p2, p3 = potential(2, t), potential(3, t)
            v1 = b0 * p2 + b1 * p3
            store(ob, 0, ch, tile, -(w0 + a1 * p2))
            store(ob, 1, ch, tile, -(w1 + a1 * p3))
            extra = load(a_ref, 0, ch, tile) * potential(4, t)
            for j in range(1, 4):
                extra = extra + load(a_ref, j, ch, tile) * potential(4 + j, t)
            store(va, 0, ch, tile, -(v0 + jnp.where(xl == 0, extra, 0.0)))
            store(va, 1, ch, tile, -(v1 + jnp.where(xl == 0, 0.0, extra)))

    def second(kind, ch, src, dst, peer, recv_kind=None):
        recv_at = CHUNKS * (kind if recv_kind is None else recv_kind) + ch
        return remote(send, recv, kind, recv_at, src, dst, peer)

    def to_far(ch):
        return second(0, ch, va.at[:, part_rows(far, ch), :], back1.at[ch], across)

    def to_core(ch):
        return second(1, ch, va.at[:, part_rows(near, ch), :], back2.at[ch], core)

    def to_diagonal(ch):
        return second(2, ch, va.at[:, part_rows(3 - g, ch), :], back3.at[ch], diagonal)

    def owed_core(j, ch):
        return second(3 + j, ch, ob.at[:, part_rows(2 * j + 1 - c, ch), :], owed1.at[ch, j], core)

    def owed(j, ch):
        return second(5 + j, ch, sums.at[ch, j], owed3.at[ch, xl], at((b + 31) % 32, 2 * j + c), 5 + xl)

    def owed_in(j, ch):
        return second(5 + j, ch, sums.at[ch, j], owed3.at[ch, j], down)

    def hand_out(ch):
        owed_core(0, ch).start()
        owed_core(1, ch).start()
        if ch == 0:
            to_far(ch).start()
            to_diagonal(ch).start()
        to_core(ch).start()

    def pass_owed(ch):
        for j in range(2):
            owed_core(j, ch).wait_recv()
            sums[ch, j] = ob[:, part_rows(2 * j + c, ch), :] + owed1[ch, j]
            owed(j, ch).start()
        if ch > 0:
            to_far(ch).start()
            to_diagonal(ch).start()

    def spread(ch, j):
        tile = 9 * ch + j
        n, slot = tile % 16, tile // 16
        source = vec.at[:, :, tile_rows(tile), :]
        target = vc.at[m, :, :, pl.ds(pl.multiple_of(8 * slot, 8), 8), :]
        return remote(vsend, vrecv, 0, slot, source, target, at(2 * n + xh, g)), n

    def spread_sent(count):
        window = vec.at[:, :, pl.ds(0, 8 * count), :]
        remote(vsend, vrecv, 0, 0, window, window, across).wait_send()

    def spread_in(slot):
        window = vc.at[0:15, :, :, pl.ds(8 * slot, 8), :]
        remote(vsend, vrecv, 0, slot, window, window, across).wait_recv()

    def collect(ch):
        for copy_of in (to_far, to_core, to_diagonal):
            copy_of(ch).wait_recv()
        for j in range(2):
            owed_in(j, ch).wait_recv()
        where = pl.ds(ch * SPAN, SPAN)
        for e in range(2):
            vec[e, c, where, :] = va[e, part_rows(g, ch), :] + back1[ch, e] + owed3[ch, c, e]
            vec[e, 1 - c, where, :] = back2[ch, e] + back3[ch, e] + owed3[ch, 1 - c, e]

        def start(k, _):
            copy, n = spread(ch, (k + m) % 9)

            @pl.when(n != m)
            def _():
                copy.start()

            return 0

        lax.fori_loop(0, 9, start, 0)
        for t in range(TILES * ch, TILES * ch + TILES):
            place = pl.ds(ch * SPAN + t % TILES, 12, stride=TILES)
            for e in range(2):
                for n in range(2):
                    v_out[pl.ds(4 * t + 2 * n + e, 12, stride=72), :] = vec[e, n, place, :]

    for ch in range(CHUNKS):
        with jax.named_scope("along_z"):
            along_z(ch, q_ref, r_ref)
        if ch > 0:
            with jax.named_scope("pass_owed"):
                pass_owed(ch - 1)
        with jax.named_scope("turn_out"):
            turn_out(ch)
        if ch > 0:
            low_chunk(ch - 1)
        with jax.named_scope("backward"):
            backward(ch)
            hand_out(ch)
    with jax.named_scope("pass_owed"):
        pass_owed(CHUNKS - 1)
        low_chunk(CHUNKS - 1)
        keep_own(low, low_m, 1 - xh)
        for sent in gathers:
            sent.wait_send()
    for ch in range(CHUNKS):
        with jax.named_scope("collect"):
            collect(ch)
    with jax.named_scope("spread_wait"):
        vc[m, :, :, 0:8, :] = vec[:, :, tile_rows(m), :]
        vc[m, :, :, 8:16, :] = vec[:, :, tile_rows(jnp.where(m <= 10, m + 16, m)), :]
        for kind, w in enumerate((va, va, va, ob, ob, sums, sums)):
            if kind < 5:
                whole = w.at[:, 0:SLAB, :]
            else:
                whole = w.at[:, 0]
            remote(send, recv, kind, kind, whole, whole, across).wait_send()
        scattered(0)
        scattered(1)

        spread_in(0)

    dims = (((1,), (1,)), ((), ()))
    o_rows, v_rows = o_all.reshape(2048, 128), vc.reshape(1024, 128)

    def products(start):
        total = jnp.zeros((64, 128), F32)
        for r in range(start, start + 8):
            oh, ol = split(o_rows[pl.ds(r, 128, stride=16), :])
            vh, vl = split(v_rows[pl.ds(r, 64, stride=16), :])
            left = jnp.concatenate([vh, vl, vh], axis=1)
            right = jnp.concatenate([oh, oh, ol], axis=1)
            total = total + lax.dot_general(left, right, dims, preferred_element_type=F32)
        return total

    with jax.named_scope("products_first"):
        summed[...] = products(0)
    with jax.named_scope("spread_last"):

        @pl.when(m <= 10)
        def _():
            spread_in(1)
            summed[...] = summed[...] + products(8)
            spread_sent(25)

        @pl.when(m > 10)
        def _():
            spread_sent(26)

    with jax.named_scope("arrange"):
        lane = lax.broadcasted_iota(jnp.int32, (16, 128), 1) // 32
        slots = (0, 2, 1, 3)
        kinds = [summed[pl.ds(k, 16, stride=4), :] * (1.0 / NCELL) for k in slots]
        for q in range(4):
            row = kinds[q]
            for k in range(4):
                if k != q:
                    row = jnp.where(lane == k, pltpu.roll(kinds[k], 32 * ((k - q) % 4), 1), row)
            for n in range(16):
                part[4 * n + q] = row[n : n + 1, :]

    def deal_start(k, _):
        n = (m + k) % 16
        for j in range(4):
            q = (g + j) % 4
            copy = remote(psend, precv, 0, 0, part.at[4 * n + q], rows_in.at[4 * k + j], at(2 * n + xh, q))
            if j > 0:
                copy.start()
            else:
                pl.when(k < 16)(copy.start)
        return 0

    with jax.named_scope("deal"):
        lax.fori_loop(1, 17, deal_start, 0)
        window = rows_in.at[4:67]
        remote(psend, precv, 0, 0, window, window, across).wait()
        terms = [part[4 * m + g]] + [rows_in[k] for k in range(4, 68) if k != 64]
        while len(terms) > 1:
            terms = [sum(terms[i + 1 : i + 4], terms[i]) for i in range(0, len(terms), 4)]
        whole = terms[0]
        for k in range(4):
            m_out[k : k + 1, :] = whole[:, 32 * k : 32 * (k + 1)]


def on_device(orbitals):
    shape = jax.ShapeDtypeStruct
    dma = pltpu.SemaphoreType.DMA

    def room(*dims):
        return pltpu.VMEM(dims, F32)

    packed = orbitals.reshape(4, SLAB, 128).transpose(1, 0, 2).reshape(4 * SLAB, 128)
    triple = room(CHUNKS, 2, SPAN, 128)
    pairs = room(CHUNKS, 2, 2, SPAN, 128)
    vectors, margin = pl.pallas_call(
        exchange_kernel,
        out_shape=(pltpu.VMEM((4 * SLAB, 128), F32), pltpu.VMEM((4, 32), F32)),
        in_specs=[pl.BlockSpec(memory_space=pltpu.HBM)] * 2,
        out_specs=(VMEM, VMEM),
        scratch_shapes=[
            room(4 * SLAB, 128), pltpu.VMEM((NG, 3 * NG), BF16), dma((2,)), room(4, SLAB, 128), room(4, SLAB, 128),
            room(4, 864, 128), room(2, 864, 128), room(16, 2, 4, 16, 128), room(3, NG * NG, 128),
            room(18, 384, 128), room(3, NG * PITCH, 128), room(3, NG * PITCH, 128),
            room(2, 864, 128), room(2, 864, 128), pairs, pairs, pairs, triple, triple, triple,
            room(2, 2, SLAB, 128), room(16, 2, 2, 16, 128), room(64, 128),
            room(64, 1, 128), room(68, 1, 128),
            dma((8,)), dma((24,)), dma((2,)), dma((2,)), dma((7,)), dma((21,)),
            dma((1,)), dma((2,)), dma((1,)), dma((1,)),
        ],
        compiler_params=pltpu.CompilerParams(
            collective_id=0, has_side_effects=True, vmem_limit_bytes=56 * 1024 * 1024
        ),
        name="exchange",
    )(
        pltpu.with_memory_space_constraint(packed, pltpu.HBM),
        pltpu.with_memory_space_constraint(hartley_rows(), pltpu.HBM),
    )
    vectors = vectors.reshape(SLAB, 4, 128).transpose(1, 0, 2).reshape(4, SLAB * 128)
    return vectors, margin.T


def solution(mesh):
    return jax.shard_map(
        on_device,
        mesh=mesh,
        in_specs=(P("band", "grid"),),
        out_specs=(P("band", "grid"), P("grid", "band")),
        check_vma=False,
    )
```

```python
import jax
import jax.numpy as jnp
import numpy as np
from jax import lax
from jax.experimental import pallas as pl
from jax.experimental.pallas import tpu as pltpu
from jax.sharding import PartitionSpec as P

NG = 48
NCELL = 110592
PITCH = 52
SLAB = 216
MESH = pl.DeviceIdType.MESH
F32 = jnp.float32
BF16 = jnp.bfloat16
CHUNKS, TILES, SPAN = 3, 6, 72
U3 = 48
VMEM = pl.BlockSpec(memory_space=pltpu.VMEM)


def hartley_rows():
    index = np.arange(NG)
    angles = (index[:, None] * index[None, :] % NG) * (2 * np.pi / NG)
    table = (np.cos(angles) + np.sin(angles)).astype(np.float32)
    high = table.astype(BF16)
    low = (table - high.astype(np.float32)).astype(BF16)
    return jnp.asarray(np.concatenate([high, high, low], axis=1))


def folded(index):
    return ((index + NG // 2) % NG - NG // 2).astype(F32)


def at(b, g):
    return {"band": b, "grid": g}


def part_rows(g, ch):
    return pl.ds(pl.multiple_of(ch * 4 * SPAN + g * SPAN, 8), SPAN)


def split(value):
    high = value.astype(BF16)
    low = (value - high.astype(F32)).astype(BF16)
    return high, low


def hartley(table, value):
    high, low = split(value)
    stack = jnp.concatenate([high, low, high], axis=0)
    dims = (((1,), (0,)), ((), ()))
    return lax.dot_general(table, stack, dims, preferred_element_type=F32)


def fill_kernel(k_ref):
    lane = lax.broadcasted_iota(jnp.int32, (1, 128), 1)
    y = folded(lax.broadcasted_iota(jnp.int32, (NG, 128), 0))
    x = [folded((l * 128 + lane) % NG) for l in range(3)]
    planes = [y * y + v * v for v in x]

    def plane(z, _):
        depth = z.astype(F32)
        depth = depth * depth
        for l in range(3):
            square = planes[l] + depth
            safe = jnp.where(square > 0, square, 1.0)
            value = (40.0 / NCELL) * (1.0 - jnp.exp(-square / 16.0)) / safe
            value = jnp.where(square > 0, value, 0.0)
            k_ref[l, pl.ds(pl.multiple_of(z * NG, 8), NG), :] = value
        return 0

    lax.fori_loop(0, NG // 2 + 1, plane, 0)

    def mirror(z, _):
        for l in range(3):
            source = pl.ds(pl.multiple_of((NG - z) * NG, 8), NG)
            k_ref[l, pl.ds(pl.multiple_of(z * NG, 8), NG), :] = k_ref[l, source, :]
        return 0

    lax.fori_loop(NG // 2 + 1, NG, mirror, 0)


def exchange_kernel(orb_hbm, h_hbm, v_out, m_out, orb, h_ref, load_sem, own, low, a_ref, b_ref, o_all, k_ref, s_ref, r_ref, q_ref,
                    va, ob, owed1, sums, owed3, back, vec, vc, summed, part, rows_in,
                    gsend, grecv, osend, orecv, send, recv, vsend, vrecv, psend, precv):
    b, g = lax.axis_index("band"), lax.axis_index("grid")
    m, xh, xl, c = b // 2, b % 2, g // 2, g % 2
    far, near = (g + 2) % 4, g + 1 - 2 * c
    across, core, diagonal = at(b, far), at(b, near), at(b, 3 - g)
    up, up_far = at((b + 1) % 32, g), at((b + 1) % 32, far)
    down, down_far = at((b + 31) % 32, g), at((b + 31) % 32, far)
    low_m = (m + 15 + xh) % 16
    fetch = pltpu.make_async_copy(orb_hbm, orb, load_sem.at[0])
    fetch.start()
    fetch_table = pltpu.make_async_copy(h_hbm, h_ref, load_sem.at[1])
    fetch_table.start()
    barrier = pltpu.get_barrier_semaphore()
    for peer in (up, up_far, down, down_far, across, core, diagonal):
        pl.semaphore_signal(barrier, inc=1, device_id=peer, device_id_type=MESH)

    def greet(k, _):
        peer = at(2 * ((m + k) % 16) + xh, g)
        pl.semaphore_signal(barrier, inc=1, device_id=peer, device_id_type=MESH)
        return 0

    lax.fori_loop(1, 16, greet, 0)
    fetch.wait()
    for n in range(4):
        for t in range(18):
            ch, tile = divmod(t, TILES)
            own[n, pl.ds(ch * SPAN + tile, 12, stride=TILES), :] = orb[pl.ds(4 * t + n, 12, stride=72), :]
    for ch in range(CHUNKS):
        a_ref[:, part_rows(g, ch), :] = own[:, ch * SPAN : (ch + 1) * SPAN, :]
    pl.semaphore_wait(barrier, 22)

    def remote(sends, recvs, sem, recv_sem, src, dst, peer):
        return pltpu.make_async_remote_copy(
            src_ref=src, dst_ref=dst, send_sem=sends.at[sem], recv_sem=recvs.at[recv_sem],
            device_id=peer, device_id_type=MESH,
        )

    def first(kind, ch, src, dst, peer):
        return remote(gsend, grecv, kind, CHUNKS * kind + ch, src, dst, peer)

    def same(kind, ch, ref, owner, peer):
        where = ref.at[:, part_rows(owner, ch), :]
        return first(kind, ch, where, where, peer)

    def a_across(ch):
        return same(0, ch, a_ref, g, across)

    def b_wide(ch):
        src = a_ref.at[pl.ds(2 * xl, 2), part_rows(g, ch), :]
        return first(1, ch, src, b_ref.at[:, part_rows(g, ch), :], up)

    def b_near(ch):
        src = a_ref.at[pl.ds(2 - 2 * xl, 2), part_rows(g, ch), :]
        return first(2, ch, src, b_ref.at[:, part_rows(g, ch), :], up_far)

    def a_core(ch):
        return same(3, ch, a_ref, g, core)

    def a_far(ch):
        return same(4, ch, a_ref, far, core)

    def b_core(ch):
        return same(5, ch, b_ref, far, core)

    def b_far(ch):
        return same(6, ch, b_ref, g, core)

    def low_across(ch):
        target = low.at[pl.ds(2 * xl, 2), pl.ds(ch * SPAN, SPAN), :]
        return first(7, ch, b_ref.at[:, part_rows(far, ch), :], target, across)

    def low_in(ch):
        target = low.at[pl.ds(2 - 2 * xl, 2), pl.ds(ch * SPAN, SPAN), :]
        return first(7, ch, b_ref.at[:, part_rows(far, ch), :], target, across)

    a_whole, b_whole, b_half = a_ref.at[:, 0:SLAB, :], b_ref.at[:, 0:SLAB, :], a_ref.at[0:2, 0:SLAB, :]
    gathers = [first(kind, 0, w, w, across) for kind, w in enumerate((a_whole, b_half, b_half, a_whole, a_whole, b_whole, b_whole, b_whole))]

    def tile_rows(tile):
        return pl.ds(pl.multiple_of(8 * tile, 8), 8)

    def scatter(source, block, half, which, ch):
        def start(k, _):
            tile = 9 * ch + (k + m) % 9
            n, slot = tile % 16, tile // 16
            target = o_all.at[block, half, :, pl.ds(pl.multiple_of(8 * slot, 8), 8), :]
            copy = remote(osend, orecv, which, which, source.at[:, tile_rows(tile), :], target, at(2 * n + xh, g))
            pl.when(n != m)(copy.start)
            return 0

        lax.fori_loop(0, 9, start, 0)

    def keep_own(source, block, half):
        o_all[block, half, :, 0:8, :] = source[:, tile_rows(m), :]
        o_all[block, half, :, 8:16, :] = source[:, tile_rows(jnp.where(m <= 10, m + 16, m)), :]

    def scattered(which):
        def wait(sent, rows):
            window = own.at[:, 0 : 8 * sent, :]
            remote(osend, orecv, which, which, window, window, across).wait_send()
            window = o_all.at[0:15, 0, :, 0:rows, :]
            remote(osend, orecv, which, which, window, window, across).wait_recv()

        @pl.when(m <= 10)
        def _():
            wait(25, 16)

        @pl.when(m > 10)
        def _():
            wait(26, 8)

    def low_chunk(ch):
        with jax.named_scope("low"):
            low_in(ch).wait_recv()
            low[pl.ds(2 * xl, 2), pl.ds(ch * SPAN, SPAN), :] = b_ref[:, part_rows(g, ch), :]
            scatter(low, low_m, 1 - xh, 1, ch)

    d = 2 * c + xl

    def rows(ch, tile):
        return pl.ds(ch * 4 * SPAN + tile, NG, stride=TILES)

    def load(ref, i, ch, tile):
        return jnp.concatenate([ref[i, rows(ch, tile), :], ref[i, rows(ch, tile + 1), :]], axis=1)

    def store(ref, j, ch, tile, value):
        ref[j, rows(ch, tile), :] = value[:, :128]
        ref[j, rows(ch, tile + 1), :] = value[:, 128:]

    def forward(ch):
        for tile in range(0, TILES, 2):
            t = ch * TILES + tile
            single = load(a_ref, d, ch, tile)
            a0, a1 = load(a_ref, 2 * c, ch, tile), load(a_ref, 2 * c + 1, ch, tile)
            b0, b1 = load(b_ref, 0, ch, tile), load(b_ref, 1, ch, tile)
            for f in range(8):
                left = (a0, a0, a1, a1)[f] if f < 4 else single
                right = (b0, b1, b0, b1)[f] if f < 4 else load(a_ref, f - 4, ch, tile)
                out = hartley(table, left * right)
                s_ref[t, f * 48 : (f + 1) * 48, :] = out[:, :128]
                s_ref[t + 1, f * 48 : (f + 1) * 48, :] = out[:, 128:]

    def block_of(n, i):
        y, z = divmod(n * 8, 48)
        return pl.ds((i * 8 + y) * PITCH + z, 8)

    def turn_in(ch):
        def step(i, _):
            for v in range(3):
                for l in range(3):
                    block = s_ref[i * 3 + v, l * 128 : (l + 1) * 128, :].T
                    for n in range(16):
                        r_ref[l, block_of(v * 16 + n, i), :] = block[n * 8 : (n + 1) * 8, :]
            return 0

        for i in (2 * ch, 2 * ch + 1):
            step(i, 0)

    def turn_out(ch):
        def step(i, _):
            for v in range(3):
                for l in range(3):
                    parts = [r_ref[l, block_of(v * 16 + n, i), :] for n in range(16)]
                    s_ref[i * 3 + v, l * 128 : (l + 1) * 128, :] = jnp.concatenate(parts, axis=0).T
            return 0

        for i in (2 * ch, 2 * ch + 1):
            step(i, 0)

    def passes(source, target, where, count, scale=None):
        tiles = [(u, l) for u in range(count) for l in range(3)]
        for p in range(0, len(tiles), 2):
            pair = tiles[p : p + 2]
            value = jnp.concatenate([source[l, where(u), :] for u, l in pair], axis=1)
            out = hartley(table, value)
            for j, (u, l) in enumerate(pair):
                piece = out[:, 128 * j : 128 * (j + 1)]
                if scale is not None:
                    piece = piece * k_ref[l, scale(u), :]
                target[l, where(u), :] = piece

    def along_z(ch, source, target):
        passes(source, target, lambda u: pl.ds((16 * ch + u) * PITCH, 48), 16)

    def along_y(source, target, scaled):
        def step(i, _):
            passes(source, target, lambda u: pl.ds(i * U3 + u, 48, stride=PITCH), U3,
                   (lambda u: pl.ds(pl.multiple_of((i * U3 + u) * 48, 8), 48)) if scaled else None)
            return 0

        lax.fori_loop(0, 48 // U3, step, 0)

    with jax.named_scope("start"):
        for ch in range(CHUNKS):
            for copy_of in (b_wide, b_near, a_across, a_core):
                copy_of(ch).start()
        keep_own(own, m, xh)
        fill_kernel(k_ref)
        fetch_table.wait()
    table = h_ref[...]
    for ch in range(CHUNKS):
        with jax.named_scope("gather"):
            b_near(ch).wait_recv()
            b_core(ch).start()
            b_wide(ch).wait_recv()
            b_far(ch).start()
            a_across(ch).wait_recv()
            a_far(ch).start()
            if ch == CHUNKS - 1:
                for early in range(CHUNKS):
                    low_across(early).start()
            for copy_of in (a_core, b_core, a_far, b_far):
                copy_of(ch).wait_recv()
        with jax.named_scope("forward"):
            forward(ch)
        with jax.named_scope("turn_in"):
            turn_in(ch)
        with jax.named_scope("along_z"):
            along_z(ch, r_ref, q_ref)
        if ch == 0:
            for part_ch in range(CHUNKS):
                scatter(own, m, xh, 0, part_ch)
    with jax.named_scope("along_y"):
        along_y(q_ref, r_ref, True)
    with jax.named_scope("along_y"):
        along_y(r_ref, q_ref, False)

    def potential(f, t):
        span = slice(f * 48, (f + 1) * 48)
        return hartley(table, jnp.concatenate([s_ref[t, span, :], s_ref[t + 1, span, :]], axis=1))

    def backward(ch):
        for tile in range(0, TILES, 2):
            t = ch * TILES + tile
            b0, b1 = load(b_ref, 0, ch, tile), load(b_ref, 1, ch, tile)
            a0, a1 = load(a_ref, 2 * c, ch, tile), load(a_ref, 2 * c + 1, ch, tile)
            p0, p1 = potential(0, t), potential(1, t)
            v0 = b0 * p0 + b1 * p1
            w0, w1 = a0 * p0, a0 * p1
            p2, p3 = potential(2, t), potential(3, t)
            v1 = b0 * p2 + b1 * p3
            store(ob, 0, ch, tile, -(w0 + a1 * p2))
            store(ob, 1, ch, tile, -(w1 + a1 * p3))
            extra = load(a_ref, 0, ch, tile) * potential(4, t)
            for j in range(1, 4):
                extra = extra + load(a_ref, j, ch, tile) * potential(4 + j, t)
            store(va, 0, ch, tile, -(v0 + jnp.where(xl == 0, extra, 0.0)))
            store(va, 1, ch, tile, -(v1 + jnp.where(xl == 0, 0.0, extra)))

    def second(kind, ch, src, dst, peer, recv_kind=None):
        recv_at = CHUNKS * (kind if recv_kind is None else recv_kind) + ch
        return remote(send, recv, kind, recv_at, src, dst, peer)

    def to_far(ch):
        return second(0, ch, va.at[:, part_rows(far, ch), :], back.at[ch, 0], across, 0)

    def to_core(ch):
        return second(1, ch, va.at[:, part_rows(near, ch), :], back.at[ch, 1], core, 0)

    def to_diagonal(ch):
        return second(2, ch, va.at[:, part_rows(3 - g, ch), :], back.at[ch, 2], diagonal, 0)

    def owed_core(j, ch):
        return second(3 + j, ch, ob.at[:, part_rows(2 * j + 1 - c, ch), :], owed1.at[ch, j], core, 1)

    def owed(j, ch):
        return second(5 + j, ch, sums.at[ch, j], owed3.at[ch, xl], at((b + 31) % 32, 2 * j + c), 2)

    def arrived(kind, ch, window):
        second(kind, ch, window, window, across).wait_recv()

    def hand_out(ch):
        owed_core(0, ch).start()
        owed_core(1, ch).start()
        if ch == 0:
            to_far(ch).start()
            to_diagonal(ch).start()
        to_core(ch).start()

    def pass_owed(ch):
        arrived(1, ch, owed1.at[ch])
        for j in range(2):
            sums[ch, j] = ob[:, part_rows(2 * j + c, ch), :] + owed1[ch, j]
            owed(j, ch).start()
        if ch > 0:
            to_far(ch).start()
            to_diagonal(ch).start()

    def spread(ch, j):
        tile = 9 * ch + j
        n, slot = tile % 16, tile // 16
        source = vec.at[:, :, tile_rows(tile), :]
        target = vc.at[m, :, :, pl.ds(pl.multiple_of(8 * slot, 8), 8), :]
        return remote(vsend, vrecv, 0, slot, source, target, at(2 * n + xh, g)), n

    def spread_sent(count):
        window = vec.at[:, :, pl.ds(0, 8 * count), :]
        remote(vsend, vrecv, 0, 0, window, window, across).wait_send()

    def spread_in(slot):
        window = vc.at[0:15, :, :, pl.ds(8 * slot, 8), :]
        remote(vsend, vrecv, 0, slot, window, window, across).wait_recv()

    def collect(ch):
        arrived(0, ch, back.at[ch])
        arrived(2, ch, owed3.at[ch])
        where = pl.ds(ch * SPAN, SPAN)
        for e in range(2):
            vec[e, c, where, :] = va[e, part_rows(g, ch), :] + back[ch, 0, e] + owed3[ch, c, e]
            vec[e, 1 - c, where, :] = back[ch, 1, e] + back[ch, 2, e] + owed3[ch, 1 - c, e]

        def start(k, _):
            copy, n = spread(ch, (k + m) % 9)

            @pl.when(n != m)
            def _():
                copy.start()

            return 0

        lax.fori_loop(0, 9, start, 0)
        for t in range(TILES * ch, TILES * ch + TILES):
            place = pl.ds(ch * SPAN + t % TILES, 12, stride=TILES)
            for e in range(2):
                for n in range(2):
                    v_out[pl.ds(4 * t + 2 * n + e, 12, stride=72), :] = vec[e, n, place, :]

    for ch in range(CHUNKS):
        with jax.named_scope("along_z"):
            along_z(ch, q_ref, r_ref)
        if ch > 0:
            with jax.named_scope("pass_owed"):
                pass_owed(ch - 1)
        with jax.named_scope("turn_out"):
            turn_out(ch)
        if ch > 0:
            low_chunk(ch - 1)
        with jax.named_scope("backward"):
            backward(ch)
            hand_out(ch)
    with jax.named_scope("pass_owed"):
        pass_owed(CHUNKS - 1)
        low_chunk(CHUNKS - 1)
        keep_own(low, low_m, 1 - xh)
        for sent in gathers:
            sent.wait_send()
    for ch in range(CHUNKS):
        with jax.named_scope("collect"):
            collect(ch)
    with jax.named_scope("spread_wait"):
        vc[m, :, :, 0:8, :] = vec[:, :, tile_rows(m), :]
        vc[m, :, :, 8:16, :] = vec[:, :, tile_rows(jnp.where(m <= 10, m + 16, m)), :]
        for kind, w in enumerate((va, va, va, ob, ob, sums, sums)):
            if kind < 5:
                whole = w.at[:, 0:SLAB, :]
            else:
                whole = w.at[:, 0]
            remote(send, recv, kind, 0, whole, whole, across).wait_send()
        scattered(0)
        scattered(1)

        spread_in(0)

    dims = (((1,), (1,)), ((), ()))
    o_rows, v_rows = o_all.reshape(2048, 128), vc.reshape(1024, 128)

    def products(start):
        total = jnp.zeros((64, 128), F32)
        for r in range(start, start + 8):
            oh, ol = split(o_rows[pl.ds(r, 128, stride=16), :])
            vh, vl = split(v_rows[pl.ds(r, 64, stride=16), :])
            left = jnp.concatenate([vh, vl, vh], axis=1)
            right = jnp.concatenate([oh, oh, ol], axis=1)
            total = total + lax.dot_general(left, right, dims, preferred_element_type=F32)
        return total

    with jax.named_scope("products_first"):
        summed[...] = products(0)
    with jax.named_scope("spread_last"):

        @pl.when(m <= 10)
        def _():
            spread_in(1)
            summed[...] = summed[...] + products(8)
            spread_sent(25)

        @pl.when(m > 10)
        def _():
            spread_sent(26)

    with jax.named_scope("arrange"):
        lane = lax.broadcasted_iota(jnp.int32, (16, 128), 1) // 32
        slots = (0, 2, 1, 3)
        kinds = [summed[pl.ds(k, 16, stride=4), :] * (1.0 / NCELL) for k in slots]
        for q in range(4):
            row = kinds[q]
            for k in range(4):
                if k != q:
                    row = jnp.where(lane == k, pltpu.roll(kinds[k], 32 * ((k - q) % 4), 1), row)
            for n in range(16):
                part[4 * n + q] = row[n : n + 1, :]

    def deal_start(k, _):
        n = (m + k) % 16
        for j in range(4):
            q = (g + j) % 4
            copy = remote(psend, precv, 0, 0, part.at[4 * n + q], rows_in.at[4 * k + j], at(2 * n + xh, q))
            if j > 0:
                copy.start()
            else:
                pl.when(k < 16)(copy.start)
        return 0

    with jax.named_scope("deal"):
        lax.fori_loop(1, 17, deal_start, 0)
        window = rows_in.at[4:67]
        remote(psend, precv, 0, 0, window, window, across).wait()
        terms = [part[4 * m + g]] + [rows_in[k] for k in range(4, 68) if k != 64]
        while len(terms) > 1:
            terms = [sum(terms[i + 1 : i + 4], terms[i]) for i in range(0, len(terms), 4)]
        whole = terms[0]
        for k in range(4):
            m_out[k : k + 1, :] = whole[:, 32 * k : 32 * (k + 1)]


def on_device(orbitals):
    shape = jax.ShapeDtypeStruct
    dma = pltpu.SemaphoreType.DMA

    def room(*dims):
        return pltpu.VMEM(dims, F32)

    packed = orbitals.reshape(4, SLAB, 128).transpose(1, 0, 2).reshape(4 * SLAB, 128)
    pairs = room(CHUNKS, 2, 2, SPAN, 128)
    vectors, margin = pl.pallas_call(
        exchange_kernel,
        out_shape=(pltpu.VMEM((4 * SLAB, 128), F32), pltpu.VMEM((4, 32), F32)),
        in_specs=[pl.BlockSpec(memory_space=pltpu.HBM)] * 2,
        out_specs=(VMEM, VMEM),
        scratch_shapes=[
            room(4 * SLAB, 128), pltpu.VMEM((NG, 3 * NG), BF16), dma((2,)), room(4, SLAB, 128), room(4, SLAB, 128),
            room(4, 864, 128), room(2, 864, 128), room(16, 2, 4, 16, 128), room(3, NG * NG, 128),
            room(18, 384, 128), room(3, NG * PITCH, 128), room(3, NG * PITCH, 128),
            room(2, 864, 128), room(2, 864, 128), pairs, pairs, pairs, room(CHUNKS, 3, 2, SPAN, 128),
            room(2, 2, SLAB, 128), room(16, 2, 2, 16, 128), room(64, 128),
            room(64, 1, 128), room(68, 1, 128),
            dma((8,)), dma((24,)), dma((2,)), dma((2,)), dma((7,)), dma((9,)),
            dma((1,)), dma((2,)), dma((1,)), dma((1,)),
        ],
        compiler_params=pltpu.CompilerParams(
            collective_id=0, has_side_effects=True, vmem_limit_bytes=56 * 1024 * 1024
        ),
        name="exchange",
    )(
        pltpu.with_memory_space_constraint(packed, pltpu.HBM),
        pltpu.with_memory_space_constraint(hartley_rows(), pltpu.HBM),
    )
    vectors = vectors.reshape(SLAB, 4, 128).transpose(1, 0, 2).reshape(4, SLAB * 128)
    return vectors, margin.T


def solution(mesh):
    return jax.shard_map(
        on_device,
        mesh=mesh,
        in_specs=(P("band", "grid"),),
        out_specs=(P("band", "grid"), P("grid", "band")),
        check_vma=False,
    )
```
